128 devices in a mesh: row: 8 (over x, core), col: 16 (over y, z).
Axes of the slice: x: 4, y: 4, z: 4, core: 2. Of those that a mesh axis runs over, the one named last changes fastest.
Arguments:
- velocity: float32 [3, 2, 128, 512, 256], P(None, None, 'row', 'col'), may hold values from -6 to 6
- register: float32 [3, 2, 128, 512, 256], P(None, None, 'row', 'col'), may hold values from -6 to 6
- offsets: int32 [256], replicated, may hold values from -2 to 2, as said below
- remesh_flag: int32 [256], replicated, may hold values from 0 to 1, as said below
- keep_blocks: int32 [16], replicated, may hold values 0 or 1
Outputs:
- velocity_next: float32 [3, 2, 128, 512, 256], P(None, None, 'row', 'col')
The draws below stay inside these ranges and needn't reach their ends.
Inputs may be any that keep to these rules, and one draw needn't show every extreme that they name: offsets[j] is 0 or has the sign of ky = j - 128. On each side of ky = 0 the planes of magnitude 1 form one run of consecutive ky, and the planes of magnitude 2 the run that follows it directly, farther from ky = 0. Each of -2, -1, 1 and 2 is carried by half of 32 to 32 planes. Each nonzero value of offsets[j] remesh_flag[j] is taken by at most 32 planes, and in every draw one of them by exactly 32 planes.
All inputs are finite; a program needn't handle non-finite values.
Results may differ from the reference program's by a relative error of at most 0.0055.
Values may be sent and summed in bfloat16 or wider, within the bound.
A program may use at most 192 MiB of HBM per device.

```python
import math
import jax
import jax.numpy as jnp
from jax import lax

NX = 512
NY = 256
NZ = 256
NZH = 128
MX = 768
MY = 384
MZ = 384
KXB = 32
NBLK = 16
SHIFT_CAP = 32


def remesh_plan(key):
    folded = jax.random.fold_in(key, 4721)
    key_counts, key_pick, key_upper, key_lower, key_flag = jax.random.split(folded, 5)
    counts = jax.random.randint(key_counts, (4,), SHIFT_CAP // 2, SHIFT_CAP + 1).astype(jnp.int32)
    chosen = jax.random.randint(key_pick, (), 0, 4).astype(jnp.int32)
    slot_order = jnp.arange(4, dtype=jnp.int32)
    counts = jnp.where(slot_order == chosen, SHIFT_CAP, counts).astype(jnp.int32)
    upper_start = jax.random.randint(key_upper, (), 1, NY // 2 - counts[2] - counts[3] + 1).astype(jnp.int32)
    lower_start = jax.random.randint(key_lower, (), 1, NY // 2 - counts[1] - counts[0] + 2).astype(jnp.int32)
    ky_values = jnp.arange(NY, dtype=jnp.int32) - NY // 2
    upper_one = (ky_values >= upper_start) & (ky_values < upper_start + counts[2])
    upper_two = (ky_values >= upper_start + counts[2]) & (ky_values < upper_start + counts[2] + counts[3])
    lower_one = (ky_values <= -lower_start) & (ky_values > -lower_start - counts[1])
    lower_two = (ky_values <= -lower_start - counts[1]) & (ky_values > -lower_start - counts[1] - counts[0])
    offsets = (upper_one.astype(jnp.int32) + 2 * upper_two.astype(jnp.int32) - lower_one.astype(jnp.int32) - 2 * lower_two.astype(jnp.int32)).astype(jnp.int32)
    values = jnp.array([-2, -1, 1, 2], dtype=jnp.int32)
    chosen_value = jnp.sum(jnp.where(slot_order == chosen, values, 0)).astype(jnp.int32)
    coins = jax.random.randint(key_flag, (NY,), 0, 4).astype(jnp.int32)
    flag = jnp.where(offsets == chosen_value, 1, jnp.where(offsets != 0, (coins < 3).astype(jnp.int32), (coins < 2).astype(jnp.int32))).astype(jnp.int32)
    return (offsets, flag)


def draw_offsets(key, part):
    return remesh_plan(key)[0]


def draw_remesh_flag(key, part):
    return remesh_plan(key)[1]


def place_ends(result, stream_key, low, top_value):
    shape = result.shape
    place = [jax.random.randint(jax.random.fold_in(stream_key, axis), (), 0, shape[axis]) for axis in range(len(shape))]
    result = result.at[tuple(place)].set(low)
    longest = shape.index(max(shape))
    place[longest] = (place[longest] + 1) % shape[longest]
    return result.at[tuple(place)].set(top_value)


def level_of(own_key, extent, cuts, low, high):
    loudness, own = 1.0, jax.random.fold_in(own_key, 6)
    for axis_at, blocks in cuts:
        draws = jnp.exp(jax.random.uniform(jax.random.fold_in(own, axis_at), (blocks,), jnp.float32, low / len(cuts), high / len(cuts)))
        loudness = loudness * jnp.repeat(draws, extent[axis_at] // blocks).reshape([-1 if axis == axis_at else 1 for axis in range(len(extent))])
    return loudness


def normal_values(rng, shape, spread, most, cuts=(), kind=jnp.bfloat16):
    entries = jax.random.normal(rng, shape, jnp.float32) * spread
    if len(cuts) > 0:
        entries = level_of(rng, shape, cuts, -0.22, 0.18) * entries
    return jnp.clip(entries, min=-most, max=most).astype(kind)


def setup_inputs(seed: int = 0) -> dict:
    splits = jax.random.split(jax.random.key(seed), 6)
    return {
        "velocity": normal_values(splits[0], (3, 2, NZH, NX, NY), 1.0, 6.0, ((2, 8), (3, 16)), jnp.float32),
        "register": normal_values(splits[1], (3, 2, NZH, NX, NY), 1.0, 6.0, ((2, 8), (3, 16)), jnp.float32),
        "offsets": draw_offsets(jax.random.fold_in(splits[5], 71), 0),
        "remesh_flag": draw_remesh_flag(jax.random.fold_in(splits[5], 71), 0),
        "keep_blocks": place_ends((jax.random.randint(splits[4], (NBLK,), 0, 4) < 3).astype(jnp.int32), jax.random.fold_in(splits[4], 1), 0, 1),
    }


SHEAR_RATE = 40.0
SHEAR_TIME = 0.3
VISCOSITY = 0.0015
TIME_STEP = 0.008
REGISTER_WEIGHT = -153.0 / 128.0
UPDATE_WEIGHT = 8.0 / 15.0
PRODUCT_PAIRS = ((0, 0), (0, 1), (0, 2), (1, 1), (1, 2), (2, 2))
PAIR_LOOKUP = ((0, 1, 2), (1, 3, 4), (2, 4, 5))
OFFSET_VALUES = (-2, -1, 1, 2)
slab_rows = 32
kz_rows = 8

def phase_angles(contracted, produced, period):
    phase_turns = jnp.mod(contracted[:, None] * produced[None, :], period)
    return phase_turns.astype(jnp.float32) * (2.0 * math.pi / period)

def complex_table(contracted, produced, period, direction):
    angles = phase_angles(contracted, produced, period)
    cosine = jnp.cos(angles)
    sine_part = direction * jnp.sin(angles)
    upper_rows = jnp.stack([cosine, sine_part], axis=1)
    lower_rows = jnp.stack([-sine_part, cosine], axis=1)
    return jnp.stack([upper_rows, lower_rows], axis=0).astype(jnp.bfloat16)

def inverse_real_table(mode_list, points, period):
    angles = phase_angles(mode_list, points, period)
    weights = jnp.where(mode_list == 0, 1.0, 2.0).astype(jnp.float32)[:, None]
    return jnp.stack([weights * jnp.cos(angles), -weights * jnp.sin(angles)], axis=0).astype(jnp.bfloat16)

def forward_real_table(points, mode_list, period):
    angles = phase_angles(points, mode_list, period)
    return jnp.stack([jnp.cos(angles), -jnp.sin(angles)], axis=1).astype(jnp.bfloat16)

def tendency_update(spectra, velocity, register, kx_values, ky_values, kz_values):
    wave_x = kx_values[None, :, None] - SHEAR_TIME * ky_values[None, None, :]
    wave_y = ky_values[None, None, :]
    wave_z = kz_values[:, None, None]
    wave_list = (wave_x, wave_y, wave_z)
    squared = wave_x * wave_x + wave_y * wave_y + wave_z * wave_z
    inverse = 1.0 / jnp.maximum(squared, 1.0)
    advect_real = [sum((wave_list[source] * spectra[PAIR_LOOKUP[target][source], 1] for source in range(3))) for target in range(3)]
    advect_imag = [-sum((wave_list[source] * spectra[PAIR_LOOKUP[target][source], 0] for source in range(3))) for target in range(3)]
    diverge_real = sum((wave_list[target] * advect_real[target] for target in range(3)))
    diverge_imag = sum((wave_list[target] * advect_imag[target] for target in range(3)))
    pressure_lift = 2.0 * SHEAR_RATE * wave_y * inverse
    results = []
    for target in range(3):
        halves = []
        for half_index, advect, diverge in ((0, advect_real, diverge_real), (1, advect_imag, diverge_imag)):
            rate_value = advect[target] - wave_list[target] * diverge * inverse
            rate_value = rate_value + wave_list[target] * pressure_lift * velocity[0, half_index]
            rate_value = rate_value - VISCOSITY * squared * velocity[target, half_index]
            if target == 1:
                rate_value = rate_value - SHEAR_RATE * velocity[0, half_index]
            increment = REGISTER_WEIGHT * register[target, half_index] + TIME_STEP * rate_value
            halves.append(velocity[target, half_index] + UPDATE_WEIGHT * increment)
        results.append(jnp.stack(halves))
    return jnp.stack(results)

def contract(formula, left_operand, right_operand):
    return jnp.einsum(formula, left_operand.astype(jnp.float32), right_operand.astype(jnp.float32), precision=lax.Precision.HIGHEST)

def reference(velocity, register, offsets, remesh_flag, keep_blocks):
    inverse_scale = 1.0 / math.sqrt(NX * NY * NZ)
    forward_scale = math.sqrt(NX * NY * NZ) / (MX * MY * MZ)
    kx_all = jnp.arange(NX, dtype=jnp.int32) - NX // 2
    ky_all = jnp.arange(NY, dtype=jnp.int32) - NY // 2
    kz_all = jnp.arange(NZH, dtype=jnp.int32)
    x_points = jnp.arange(MX, dtype=jnp.int32)
    y_points = jnp.arange(MY, dtype=jnp.int32)
    z_points = jnp.arange(MZ, dtype=jnp.int32)
    y_inverse = complex_table(ky_all, y_points, MY, 1.0)
    x_inverse = complex_table(kx_all, x_points, MX, 1.0)
    z_inverse = inverse_real_table(kz_all, z_points, MZ)
    z_forward = forward_real_table(z_points, kz_all, MZ)
    x_forward = complex_table(x_points, kx_all, MX, -1.0)
    y_forward = complex_table(y_points, ky_all, MY, -1.0)
    collected = []
    for component in range(3):
        spectral = velocity[component].astype(jnp.bfloat16)
        along_y = contract('rlij,rjsq->slqi', spectral, y_inverse).astype(jnp.bfloat16)
        collected.append(contract('rlqi,risp->slqp', along_y, x_inverse).astype(jnp.bfloat16))
    grids = jnp.stack(collected)

    def slab_products(start):
        section = lax.dynamic_slice_in_dim(grids, start, slab_rows, 3)
        fields = contract('crlqp,rlz->cqpz', section, z_inverse) * inverse_scale
        products = jnp.stack([fields[left_factor] * fields[right_factor] for left_factor, right_factor in PRODUCT_PAIRS]).astype(jnp.bfloat16)
        modes_z = contract('eqpz,zsl->esqpl', products, z_forward).astype(jnp.bfloat16)
        return contract('erqpl,rpsi->esqil', modes_z, x_forward).astype(jnp.bfloat16)
    slabs = lax.map(slab_products, jnp.arange(MY // slab_rows, dtype=jnp.int32) * slab_rows)
    modes_x = jnp.moveaxis(slabs, 0, 2).reshape(6, 2, MY, NX, NZH)

    def kz_update(start):
        section = lax.dynamic_slice_in_dim(modes_x, start, kz_rows, 4)
        spectra = contract('erqil,rqsj->eslij', section, y_forward) * forward_scale
        velocity_part = lax.dynamic_slice_in_dim(velocity, start, kz_rows, 2)
        register_part = lax.dynamic_slice_in_dim(register, start, kz_rows, 2)
        kz_values = (start + jnp.arange(kz_rows, dtype=jnp.int32)).astype(jnp.float32)
        return tendency_update(spectra, velocity_part, register_part, kx_all.astype(jnp.float32), ky_all.astype(jnp.float32), kz_values)
    updates = lax.map(kz_update, jnp.arange(NZH // kz_rows, dtype=jnp.int32) * kz_rows)
    updated = jnp.moveaxis(updates, 0, 2).reshape(3, 2, NZH, NX, NY)
    moved_by = offsets * remesh_flag
    remeshed = updated * (moved_by == 0).astype(jnp.float32)
    for shift_by in OFFSET_VALUES:
        selected = updated * (moved_by == shift_by).astype(jnp.float32)
        amount = shift_by * KXB
        if amount > 0:
            selected = jnp.pad(selected[:, :, :, :NX - amount], ((0, 0), (0, 0), (0, 0), (amount, 0), (0, 0)))
        else:
            selected = jnp.pad(selected[:, :, :, -amount:], ((0, 0), (0, 0), (0, 0), (0, -amount), (0, 0)))
        remeshed = remeshed + selected
    block_keep = keep_blocks[jnp.arange(NX, dtype=jnp.int32) // KXB].astype(jnp.float32)
    return remeshed * block_keep[None, None, None, :, None]
```

```python
import math

import jax
import jax.numpy as jnp
import numpy as np
from jax import lax
from jax.experimental import pallas as pl
from jax.experimental.pallas import tpu as pltpu
from jax.sharding import PartitionSpec as P

NX, NY, NZ, NZH = 512, 256, 256, 128
MX, MY, MZ = 768, 384, 384
SHIFT_CAP = 32
ROWS, COLS = 8, 16
DEVICES = ROWS * COLS
PLANES = MY // DEVICES
KZL = NZH // ROWS
KXL = NX // COLS
MODES = KZL * KXL
PRODUCTS = 5

SHEAR_RATE = 40.0
SHEAR_TIME = 0.3
VISCOSITY = 0.0015
TIME_STEP = 0.008
REGISTER_WEIGHT = -153.0 / 128.0
UPDATE_WEIGHT = 8.0 / 15.0
OFFSET_VALUES = (-2, -1, 1, 2)
INVERSE_SCALE = 1.0 / math.sqrt(NX * NY * NZ)
FORWARD_SCALE = math.sqrt(NX * NY * NZ) / (MX * MY * MZ)

F32, BF16 = jnp.float32, jnp.bfloat16
NN = (((1,), (0,)), ((), ()))
NT = (((1,), (1,)), ((), ()))


def dot(a, b, dims=NN):
    return lax.dot_general(a, b, dims, preferred_element_type=F32)


def cos_sin(left, right, period):
    turns = np.mod(np.outer(left, right), period)
    angles = turns.astype(np.float32) * np.float32(2.0 * math.pi / period)
    return np.cos(angles), np.sin(angles)


def tables():
    kx = np.arange(NX) - NX // 2
    ky = np.arange(NY) - NY // 2
    quarter, row, four = np.meshgrid(np.arange(4), np.arange(ROWS), np.arange(4), indexing="ij")
    kz = (row * KZL + four * 4 + quarter).reshape(-1)

    def mixed(re, im, axis):
        out = np.stack([re, im], axis=axis + 1)
        shape = list(re.shape)
        shape[axis] *= 2
        return out.reshape(shape)

    c, s = cos_sin(np.arange(MY), ky, MY)
    y_inv = np.stack([np.concatenate([c, -s], 1), np.concatenate([s, c], 1)])
    c, s = cos_sin(kx, np.arange(MX), MX)
    x_inv = np.concatenate([c, s], 1)
    x_fwd = np.concatenate([c.T, s.T], 0)
    c, s = cos_sin(np.arange(MZ), kz, MZ)
    w = np.where(kz == 0, 1.0, 2.0).astype(np.float32)[None]
    z_inv = np.concatenate([mixed(w * c, -w * s, 1), mixed(-w * s, -w * c, 1)], 1)
    z_fwd = np.concatenate([mixed(c.T, -s.T, 0), mixed(-s.T, -c.T, 0)], 0)
    c, s = cos_sin(ky, np.arange(MY), MY)
    c = c.reshape(NY, PLANES, DEVICES)
    s = s.reshape(NY, PLANES, DEVICES)
    y_fwd = np.concatenate([np.stack([c, s], 2), np.stack([-s, c], 2)], 0)
    y_fwd = y_fwd.reshape(2 * NY, 2 * MY)
    return [t.astype(jnp.bfloat16) for t in (y_inv, x_inv, z_inv, z_fwd, x_fwd, y_fwd)]


def lane_blocks(parts):
    lane = lax.broadcasted_iota(jnp.int32, parts[0].shape, 1)
    low_half = lane < 64
    even = (lane // 32) % 2 == 0
    a, b, c, d = parts
    roll = lambda x, n: pltpu.roll(x, n, 1)
    a, c = jnp.where(low_half, a, roll(c, 64)), jnp.where(low_half, roll(a, 64), c)
    b, d = jnp.where(low_half, b, roll(d, 64)), jnp.where(low_half, roll(b, 64), d)
    a, b = jnp.where(even, a, roll(b, 32)), jnp.where(even, roll(a, 96), b)
    c, d = jnp.where(even, c, roll(d, 32)), jnp.where(even, roll(c, 96), d)
    return a, b, c, d


def y_inverse_kernel(v_ref, t_ref, out_ref, both, grid):
    both[:, :NY] = v_ref[0, 0].astype(BF16)
    both[:, NY:] = v_ref[0, 1].astype(BF16)
    for q in range(PLANES):
        for s in range(2):
            for h in range(2):
                part = dot(t_ref[s, q * DEVICES:(q + 1) * DEVICES, :], both[h * 256:(h + 1) * 256, :], NT)
                for k in range(2):
                    grid[pl.ds((2 * h + k) * 2 + s, DEVICES, stride=8), :] = part[:, k * 128:(k + 1) * 128]
        out_ref[:, q, 0] = grid[...].reshape(DEVICES, 8, 128).astype(BF16)


def middle_kernel(in_ref, xi_ref, zi_ref, zf_ref, xf_ref, out_ref, lines, waves, modes):
    for c in range(3):
        for g in range(4):
            parts = [in_ref[:, 4 * g + k, 0, c].reshape(64, 128).astype(F32) for k in range(4)]
            for k, part in enumerate(lane_blocks(parts)):
                lines[c, k * 64:(k + 1) * 64, g * 128:(g + 1) * 128] = part.astype(BF16)
    for c in range(3):
        for half in range(2):
            waves[c, half * 256:(half + 1) * 256, :] = dot(
                lines[c], xi_ref[:, half * MX:(half + 1) * MX]
            ).astype(BF16)
    for t in range(3):
        cols = slice(t * 256, (t + 1) * 256)
        f0, f1, f2 = [dot(zi_ref[...], waves[c, :, cols]) * INVERSE_SCALE for c in range(3)]
        products = (f0 * f0 - f1 * f1, f0 * f1, f0 * f2, f1 * f2, f2 * f2 - f1 * f1)
        for e, product in enumerate(products):
            both = dot(zf_ref[...], product.astype(BF16)).astype(BF16)
            modes[e, :, cols] = both[:256]
            modes[e, :, slice(MX + t * 256, MX + (t + 1) * 256)] = both[256:]
    for e in range(PRODUCTS):
        out = dot(modes[e], xf_ref[...])
        for g in range(4):
            parts = [out[k * 64:(k + 1) * 64, g * 128:(g + 1) * 128] for k in range(4)]
            for k, part in enumerate(lane_blocks(parts)):
                out_ref[:, 4 * g + k, 0, e] = part.astype(BF16).reshape(ROWS, 8, 128)


def placing_matrix(moved):
    line = lax.broadcasted_iota(jnp.int32, (128, NY), 0)
    which = line // SHIFT_CAP
    value = jnp.where(which < 2, which - 2, which - 1)
    marked = jnp.broadcast_to(moved, (128, NY)) == value
    upto = lax.broadcasted_iota(jnp.int32, (NY, NY), 0) <= lax.broadcasted_iota(jnp.int32, (NY, NY), 1)
    rank = dot(jnp.where(marked, 1.0, 0.0).astype(BF16), jnp.where(upto, 1.0, 0.0).astype(BF16))
    slot = (line % SHIFT_CAP + 1).astype(F32)
    return jnp.where(marked & (rank == slot), 1.0, 0.0).astype(BF16)


def waves_of(kx, ky, kz):
    k1 = kx - SHEAR_TIME * ky
    squared = k1 * k1 + ky * ky + kz * kz
    return k1, squared, 1.0 / jnp.maximum(squared, 1.0)


def update_kernel(in_ref, yf_ref, v_ref, r_ref, off_ref, flag_ref, out_ref, pack_ref, grid, lines, spectra, rates):
    row0 = lax.axis_index("row") * KZL
    col0 = lax.axis_index("col") * KXL - NX // 2
    for e in range(PRODUCTS):
        for q in range(PLANES):
            grid[...] = in_ref[:, q, e].reshape(8 * DEVICES, 128).astype(F32)
            for j in range(4):
                for s in range(2):
                    lines[e, (2 * q + s) * 128:(2 * q + s + 1) * 128, j * 128:(j + 1) * 128] = grid[
                        pl.ds(2 * j + s, DEVICES, stride=8), :
                    ].astype(BF16)
    scale = TIME_STEP * FORWARD_SCALE
    for h in range(2):
        cols = slice(h * 256, (h + 1) * 256)
        for e in range(PRODUCTS):
            spectra[e] = dot(yf_ref[...], lines[e, :, cols])

        def project(b, carry):
            y0 = pl.multiple_of(b * 16, 16)
            shape = (16, 256)
            ky = (lax.broadcasted_iota(jnp.int32, shape, 0) + (y0 - NY // 2)).astype(F32)
            n = lax.broadcasted_iota(jnp.int32, shape, 1)
            kx = (n % KXL + col0).astype(F32)
            kz = (n // KXL + (row0 + h * 8)).astype(F32)
            k1, squared, inv = waves_of(kx, ky, kz)
            for r in range(2):
                part = spectra.at[:, pl.ds((1 - r) * NY + y0, 16), :]
                sign = scale if r == 0 else -scale
                s0, s1, s2, s3, s4 = [part[e] * sign for e in range(PRODUCTS)]
                a0 = k1 * s0 + ky * s1 + kz * s2
                a1 = k1 * s1 + kz * s3
                a2 = k1 * s2 + ky * s3 + kz * s4
                div = (k1 * a0 + ky * a1 + kz * a2) * inv
                rates[r, pl.ds(y0, 16), :] = a0 - k1 * div
                rates[2 + r, pl.ds(y0, 16), :] = a1 - ky * div
                rates[4 + r, pl.ds(y0, 16), :] = a2 - kz * div
            return carry

        lax.fori_loop(0, NY // 16, project, 0)
        for m in range(3):
            for r in range(2):
                out_ref[m, r, cols, :] = rates[2 * m + r].T

    def finish(b, carry):
        n0 = pl.multiple_of(b * KXL, KXL)
        shape = (KXL, NY)
        ky = (lax.broadcasted_iota(jnp.int32, shape, 1) - NY // 2).astype(F32)
        kx = (lax.broadcasted_iota(jnp.int32, shape, 0) + col0).astype(F32)
        kz = (row0 + b).astype(F32)
        k1, squared, inv = waves_of(kx, ky, kz)
        lift = (2.0 * SHEAR_RATE * TIME_STEP) * ky * inv
        damp = (VISCOSITY * TIME_STEP) * squared
        for r in range(2):
            v0 = v_ref[0, r, pl.ds(n0, KXL), :]
            for m, k in enumerate((k1, ky, kz)):
                v = v_ref[m, r, pl.ds(n0, KXL), :]
                rate = out_ref[m, r, pl.ds(n0, KXL), :] + k * lift * v0 - damp * v
                if m == 1:
                    rate = rate - (SHEAR_RATE * TIME_STEP) * v0
                rate = rate + REGISTER_WEIGHT * r_ref[m, r, pl.ds(n0, KXL), :]
                out_ref[m, r, pl.ds(n0, KXL), :] = v + UPDATE_WEIGHT * rate
        return carry

    lax.fori_loop(0, KZL, finish, 0)
    placing = placing_matrix(off_ref[...] * flag_ref[...])
    for m in range(3):
        for r in range(2):
            packed = dot(out_ref[m, r].astype(BF16), placing, NT)
            parts = [packed[k * 128:(k + 1) * 128] for k in range(4)]
            for k, part in enumerate(lane_blocks(parts)):
                pack_ref[k, 2 * m + r] = part.astype(BF16)


def remesh_kernel(u_ref, *rest):
    arrived, (off_ref, flag_ref, keep_ref, out_ref) = rest[:4], rest[4:]
    moved = off_ref[...] * flag_ref[...]
    placing = placing_matrix(moved)
    stays = (moved == 0).astype(F32)
    block = lax.broadcasted_iota(jnp.int32, (1, COLS), 1)
    keep = jnp.sum(jnp.where(block == lax.axis_index("col"), keep_ref[...], 0).astype(F32), axis=1, keepdims=True)
    for m in range(3):
        for r in range(2):
            parts = lane_blocks([a[2 * m + r].astype(F32) for a in arrived])
            for k, part in enumerate(parts):
                rows = slice(k * 128, (k + 1) * 128)
                came = dot(part.astype(BF16), placing)
                out_ref[m, r, rows, :] = (u_ref[m, r, rows, :] * stays + came) * keep


def params(**more):
    return pltpu.CompilerParams(vmem_limit_bytes=60 << 20, **more)


def whole(*shape):
    return pl.BlockSpec(shape, lambda *_: (0,) * len(shape))


def local(velocity, register, offsets, remesh_flag, keep_blocks):
    y_inv, x_inv, z_inv, z_fwd, x_fwd, y_fwd = tables()
    velocity = velocity.reshape(3, 2, MODES, NY)
    register = register.reshape(3, 2, MODES, NY)
    offsets = offsets.reshape(1, NY)
    remesh_flag = remesh_flag.reshape(1, NY)
    keep_blocks = keep_blocks.reshape(1, COLS)

    sent = pl.pallas_call(
        y_inverse_kernel,
        grid=(3,),
        in_specs=[
            pl.BlockSpec((1, 2, MODES, NY), lambda c: (c, 0, 0, 0)),
            whole(2, MY, 2 * NY),
        ],
        out_specs=pl.BlockSpec((DEVICES, PLANES, 1, 8, 128), lambda c: (0, 0, c, 0, 0)),
        out_shape=jax.ShapeDtypeStruct((DEVICES, PLANES, 3, 8, 128), BF16),
        scratch_shapes=[pltpu.VMEM((MODES, 2 * NY), BF16), pltpu.VMEM((8 * DEVICES, 128), F32)],
        compiler_params=params(),
        name="y_inverse",
    )(velocity, y_inv)
    came = lax.all_to_all(sent, ("row", "col"), split_axis=0, concat_axis=0, tiled=True)
    came = came.reshape(ROWS, COLS, PLANES, 3, 8, 128)

    sent = pl.pallas_call(
        middle_kernel,
        grid=(PLANES,),
        in_specs=[
            pl.BlockSpec((ROWS, COLS, 1, 3, 8, 128), lambda q: (0, 0, q, 0, 0, 0)),
            whole(NX, 2 * MX),
            whole(MZ, 512),
            whole(512, MZ),
            whole(2 * MX, NX),
        ],
        out_specs=pl.BlockSpec((ROWS, COLS, 1, PRODUCTS, 8, 128), lambda q: (0, 0, q, 0, 0, 0)),
        out_shape=jax.ShapeDtypeStruct((ROWS, COLS, PLANES, PRODUCTS, 8, 128), BF16),
        scratch_shapes=[
            pltpu.VMEM((3, 256, NX), BF16),
            pltpu.VMEM((3, 512, MX), BF16),
            pltpu.VMEM((PRODUCTS, 256, 2 * MX), BF16),
        ],
        compiler_params=params(),
        name="middle",
    )(came, x_inv, z_inv, z_fwd, x_fwd)
    sent = sent.reshape(DEVICES, PLANES, PRODUCTS, 8, 128)
    came = lax.all_to_all(sent, ("row", "col"), split_axis=0, concat_axis=0, tiled=True)

    vmem = pl.BlockSpec(memory_space=pltpu.VMEM)
    updated, packed = pl.pallas_call(
        update_kernel,
        in_specs=[vmem] * 6,
        out_specs=(vmem, vmem),
        out_shape=(
            jax.ShapeDtypeStruct((3, 2, MODES, NY), F32),
            jax.ShapeDtypeStruct((4, 6, 128, 128), BF16),
        ),
        scratch_shapes=[
            pltpu.VMEM((8 * DEVICES, 128), F32),
            pltpu.VMEM((PRODUCTS, 2 * MY, MODES), BF16),
            pltpu.VMEM((PRODUCTS, 2 * NY, 256), F32),
            pltpu.VMEM((6, NY, 256), F32),
        ],
        compiler_params=params(),
        name="update",
    )(came, y_fwd, velocity, register, offsets, remesh_flag)

    arrived = []
    for place, distance in enumerate(OFFSET_VALUES):
        route = [(i - distance, i) for i in range(COLS) if 0 <= i - distance < COLS]
        arrived.append(lax.ppermute(packed[place], "col", route))

    out = pl.pallas_call(
        remesh_kernel,
        in_specs=[vmem] * 8,
        out_specs=vmem,
        out_shape=jax.ShapeDtypeStruct((3, 2, MODES, NY), F32),
        compiler_params=params(),
        name="remesh",
    )(updated, *arrived, offsets, remesh_flag, keep_blocks)
    return out.reshape(3, 2, KZL, KXL, NY)


def solution(mesh):
    placed = (P(None, None, "row", "col", None), P(None, None, "row", "col", None), P(), P(), P())
    return jax.shard_map(
        local,
        mesh=mesh,
        in_specs=placed,
        out_specs=P(None, None, "row", "col", None),
        check_vma=False,
    )
```

```python
import math

import jax
import jax.numpy as jnp
import numpy as np
from jax import lax
from jax.experimental import pallas as pl
from jax.experimental.pallas import tpu as pltpu
from jax.sharding import PartitionSpec as P

NX, NY, NZ, NZH = 512, 256, 256, 128
MX, MY, MZ = 768, 384, 384
SHIFT_CAP = 32
ROWS, COLS = 8, 16
DEVICES = ROWS * COLS
PLANES = MY // DEVICES
KZL = NZH // ROWS
KXL = NX // COLS
MODES = KZL * KXL
PRODUCTS = 5

SHEAR_RATE = 40.0
SHEAR_TIME = 0.3
VISCOSITY = 0.0015
TIME_STEP = 0.008
REGISTER_WEIGHT = -153.0 / 128.0
UPDATE_WEIGHT = 8.0 / 15.0
OFFSET_VALUES = (-2, -1, 1, 2)
INVERSE_SCALE = 1.0 / math.sqrt(NX * NY * NZ)
FORWARD_SCALE = math.sqrt(NX * NY * NZ) / (MX * MY * MZ)

F32, BF16 = jnp.float32, jnp.bfloat16
NN = (((1,), (0,)), ((), ()))
NT = (((1,), (1,)), ((), ()))


def dot(a, b, dims=NN):
    return lax.dot_general(a, b, dims, preferred_element_type=F32)


def cos_sin(left, right, period):
    turns = np.mod(np.outer(left, right), period)
    angles = turns.astype(np.float32) * np.float32(2.0 * math.pi / period)
    return np.cos(angles), np.sin(angles)


def tables():
    kx = np.arange(NX) - NX // 2
    ky = np.arange(NY) - NY // 2
    quarter, row, four = np.meshgrid(np.arange(4), np.arange(ROWS), np.arange(4), indexing="ij")
    kz = (row * KZL + four * 4 + quarter).reshape(-1)

    def mixed(re, im, axis):
        out = np.stack([re, im], axis=axis + 1)
        shape = list(re.shape)
        shape[axis] *= 2
        return out.reshape(shape)

    c, s = cos_sin(np.arange(MY), ky, MY)
    y_inv = np.stack([np.concatenate([c, -s], 1), np.concatenate([s, c], 1)])
    c, s = cos_sin(kx, np.arange(MX), MX)
    x_inv = np.concatenate([c, s], 1)
    x_fwd = np.concatenate([c.T, s.T], 0)
    c, s = cos_sin(np.arange(MZ), kz, MZ)
    w = np.where(kz == 0, 1.0, 2.0).astype(np.float32)[None]
    z_inv = np.concatenate([mixed(w * c, -w * s, 1), mixed(-w * s, -w * c, 1)], 1)
    z_fwd = np.concatenate([mixed(c.T, -s.T, 0), mixed(-s.T, -c.T, 0)], 0)
    c, s = cos_sin(ky, np.arange(MY), MY)
    c = c.reshape(NY, PLANES, DEVICES)
    s = s.reshape(NY, PLANES, DEVICES)
    y_fwd = np.concatenate([np.stack([c, s], 2), np.stack([-s, c], 2)], 0)
    y_fwd = y_fwd.reshape(2 * NY, 2 * MY)
    return [t.astype(jnp.bfloat16) for t in (y_inv, x_inv, z_inv, z_fwd, x_fwd, y_fwd)]


def lane_blocks(parts):
    lane = lax.broadcasted_iota(jnp.int32, parts[0].shape, 1)
    low_half = lane < 64
    even = (lane // 32) % 2 == 0
    a, b, c, d = parts
    roll = lambda x, n: pltpu.roll(x, n, 1)
    a, c = jnp.where(low_half, a, roll(c, 64)), jnp.where(low_half, roll(a, 64), c)
    b, d = jnp.where(low_half, b, roll(d, 64)), jnp.where(low_half, roll(b, 64), d)
    a, b = jnp.where(even, a, roll(b, 32)), jnp.where(even, roll(a, 96), b)
    c, d = jnp.where(even, c, roll(d, 32)), jnp.where(even, roll(c, 96), d)
    return a, b, c, d


def y_inverse_kernel(v_ref, t_ref, out_ref, both, grid):
    both[:, :NY] = v_ref[0, 0].astype(BF16)
    both[:, NY:] = v_ref[0, 1].astype(BF16)
    for q in range(PLANES):
        for s in range(2):
            for h in range(2):
                part = dot(t_ref[s, q * DEVICES:(q + 1) * DEVICES, :], both[h * 256:(h + 1) * 256, :], NT)
                for k in range(2):
                    grid[pl.ds((2 * h + k) * 2 + s, DEVICES, stride=8), :] = part[:, k * 128:(k + 1) * 128]
        out_ref[:, q, 0] = grid[...].reshape(DEVICES, 8, 128).astype(BF16)


def middle_kernel(in_ref, xi_ref, zi_ref, zf_ref, xf_ref, out_ref, lines, waves, modes):
    for c in range(3):
        for g in range(4):
            parts = [in_ref[:, 4 * g + k, 0, c].reshape(64, 128).astype(F32) for k in range(4)]
            for k, part in enumerate(lane_blocks(parts)):
                lines[c, k * 64:(k + 1) * 64, g * 128:(g + 1) * 128] = part.astype(BF16)
    for c in range(3):
        for half in range(2):
            waves[c, half * 256:(half + 1) * 256, :] = dot(
                lines[c], xi_ref[:, half * MX:(half + 1) * MX]
            ).astype(BF16)
    for t in range(3):
        cols = slice(t * 256, (t + 1) * 256)
        f0, f1, f2 = [dot(zi_ref[...], waves[c, :, cols]) * INVERSE_SCALE for c in range(3)]
        products = (f0 * f0 - f1 * f1, f0 * f1, f0 * f2, f1 * f2, f2 * f2 - f1 * f1)
        for e, product in enumerate(products):
            both = dot(zf_ref[...], product.astype(BF16)).astype(BF16)
            modes[e, :, cols] = both[:256]
            modes[e, :, slice(MX + t * 256, MX + (t + 1) * 256)] = both[256:]
    for e in range(PRODUCTS):
        out = dot(modes[e], xf_ref[...])
        for g in range(4):
            parts = [out[k * 64:(k + 1) * 64, g * 128:(g + 1) * 128] for k in range(4)]
            for k, part in enumerate(lane_blocks(parts)):
                out_ref[:, 4 * g + k, 0, e] = part.astype(BF16).reshape(ROWS, 8, 128)


def placing_matrix(moved):
    line = lax.broadcasted_iota(jnp.int32, (128, NY), 0)
    which = line // SHIFT_CAP
    value = jnp.where(which < 2, which - 2, which - 1)
    marked = jnp.broadcast_to(moved, (128, NY)) == value
    upto = lax.broadcasted_iota(jnp.int32, (NY, NY), 0) <= lax.broadcasted_iota(jnp.int32, (NY, NY), 1)
    rank = dot(jnp.where(marked, 1.0, 0.0).astype(BF16), jnp.where(upto, 1.0, 0.0).astype(BF16))
    slot = (line % SHIFT_CAP + 1).astype(F32)
    return jnp.where(marked & (rank == slot), 1.0, 0.0).astype(BF16)


def waves_of(kx, ky, kz):
    k1 = kx - SHEAR_TIME * ky
    squared = k1 * k1 + ky * ky + kz * kz
    return k1, squared, 1.0 / jnp.maximum(squared, 1.0)


def update_kernel(in_ref, yf_ref, v_ref, r_ref, off_ref, flag_ref, out_ref, pack_ref, grid, lines, spectra, rates):
    row0 = lax.axis_index("row") * KZL
    col0 = lax.axis_index("col") * KXL - NX // 2
    for e in range(PRODUCTS):
        for q in range(PLANES):
            grid[...] = in_ref[:, q, e].reshape(8 * DEVICES, 128).astype(F32)
            for j in range(4):
                for s in range(2):
                    lines[e, (2 * q + s) * 128:(2 * q + s + 1) * 128, j * 128:(j + 1) * 128] = grid[
                        pl.ds(2 * j + s, DEVICES, stride=8), :
                    ].astype(BF16)
    scale = TIME_STEP * FORWARD_SCALE
    for h in range(2):
        cols = slice(h * 256, (h + 1) * 256)
        for e in range(PRODUCTS):
            spectra[e] = dot(yf_ref[...], lines[e, :, cols])

        def project(b, carry):
            y0 = pl.multiple_of(b * 16, 16)
            shape = (16, 256)
            ky = (lax.broadcasted_iota(jnp.int32, shape, 0) + (y0 - NY // 2)).astype(F32)
            n = lax.broadcasted_iota(jnp.int32, shape, 1)
            kx = (n % KXL + col0).astype(F32)
            kz = (n // KXL + (row0 + h * 8)).astype(F32)
            k1, squared, inv = waves_of(kx, ky, kz)
            for r in range(2):
                part = spectra.at[:, pl.ds((1 - r) * NY + y0, 16), :]
                sign = scale if r == 0 else -scale
                s0, s1, s2, s3, s4 = [part[e] * sign for e in range(PRODUCTS)]
                a0 = k1 * s0 + ky * s1 + kz * s2
                a1 = k1 * s1 + kz * s3
                a2 = k1 * s2 + ky * s3 + kz * s4
                div = (k1 * a0 + ky * a1 + kz * a2) * inv
                rates[r, pl.ds(y0, 16), :] = a0 - k1 * div
                rates[2 + r, pl.ds(y0, 16), :] = a1 - ky * div
                rates[4 + r, pl.ds(y0, 16), :] = a2 - kz * div
            return carry

        lax.fori_loop(0, NY // 16, project, 0)
        for m in range(3):
            for r in range(2):
                out_ref[m, r, cols, :] = rates[2 * m + r].T

    def finish(b, carry):
        n0 = pl.multiple_of(b * KXL, KXL)
        shape = (KXL, NY)
        ky = (lax.broadcasted_iota(jnp.int32, shape, 1) - NY // 2).astype(F32)
        kx = (lax.broadcasted_iota(jnp.int32, shape, 0) + col0).astype(F32)
        kz = (row0 + b).astype(F32)
        k1, squared, inv = waves_of(kx, ky, kz)
        lift = (2.0 * SHEAR_RATE * TIME_STEP) * ky * inv
        damp = (VISCOSITY * TIME_STEP) * squared
        for r in range(2):
            v0 = v_ref[0, r, pl.ds(n0, KXL), :]
            for m, k in enumerate((k1, ky, kz)):
                v = v_ref[m, r, pl.ds(n0, KXL), :]
                rate = out_ref[m, r, pl.ds(n0, KXL), :] + k * lift * v0 - damp * v
                if m == 1:
                    rate = rate - (SHEAR_RATE * TIME_STEP) * v0
                rate = rate + REGISTER_WEIGHT * r_ref[m, r, pl.ds(n0, KXL), :]
                out_ref[m, r, pl.ds(n0, KXL), :] = v + UPDATE_WEIGHT * rate
        return carry

    lax.fori_loop(0, KZL, finish, 0)
    placing = placing_matrix(off_ref[...] * flag_ref[...])
    for m in range(3):
        for r in range(2):
            packed = dot(out_ref[m, r].astype(BF16), placing, NT)
            parts = [packed[k * 128:(k + 1) * 128] for k in range(4)]
            for k, part in enumerate(lane_blocks(parts)):
                pack_ref[k, 2 * m + r] = part.astype(BF16)


def remesh_kernel(u_ref, *rest):
    arrived, (off_ref, flag_ref, keep_ref, out_ref) = rest[:4], rest[4:]
    moved = off_ref[...] * flag_ref[...]
    placing = placing_matrix(moved)
    stays = (moved == 0).astype(F32)
    block = lax.broadcasted_iota(jnp.int32, (1, COLS), 1)
    keep = jnp.sum(jnp.where(block == lax.axis_index("col"), keep_ref[...], 0).astype(F32), axis=1, keepdims=True)
    for m in range(3):
        for r in range(2):
            parts = lane_blocks([a[2 * m + r].astype(F32) for a in arrived])
            for k, part in enumerate(parts):
                rows = slice(k * 128, (k + 1) * 128)
                came = dot(part.astype(BF16), placing)
                out_ref[m, r, rows, :] = (u_ref[m, r, rows, :] * stays + came) * keep


def coordinates(device):
    return device // COLS, lax.rem(device, COLS)


def exchange_kernel(in_ref, out_ref, send, recv):
    row, col = lax.axis_index("row"), lax.axis_index("col")
    me = row * COLS + col
    x, core, y, z = row // 2, lax.rem(row, 2), col // 4, lax.rem(col, 4)

    def peer(i):
        to_row = lax.rem(x + lax.rem(i, 4), 4) * 2 + lax.rem(core + i // 64, 2)
        to_col = lax.rem(y + lax.rem(i // 4, 4), 4) * 4 + lax.rem(z + lax.rem(i // 16, 4), 4)
        return to_row, to_col

    barrier = pltpu.get_barrier_semaphore()

    def greet(i, carry):
        pl.semaphore_signal(barrier, inc=1, device_id=peer(i), device_id_type=pl.DeviceIdType.MESH)
        return carry

    lax.fori_loop(1, DEVICES, greet, 0)
    pl.semaphore_wait(barrier, DEVICES - 1)
    for q in range(PLANES):

        def push(i, carry):
            to = peer(i)
            pltpu.make_async_remote_copy(
                src_ref=in_ref.at[to[0] * COLS + to[1], q],
                dst_ref=out_ref.at[me, q],
                send_sem=send.at[q],
                recv_sem=recv.at[q],
                device_id=to,
                device_id_type=pl.DeviceIdType.MESH,
            ).start()
            return carry

        lax.fori_loop(1, DEVICES, push, 0)
    out_ref[me] = in_ref[me]
    for q in range(PLANES):
        arrived = out_ref.at[pl.ds(0, DEVICES - 1), q]
        pltpu.make_async_copy(arrived, arrived, recv.at[q]).wait()
        gone = in_ref.at[pl.ds(0, DEVICES - 1), q]
        pltpu.make_async_copy(gone, gone, send.at[q]).wait()


def exchange(sent, number):
    vmem = pl.BlockSpec(memory_space=pltpu.VMEM)
    return pl.pallas_call(
        exchange_kernel,
        in_specs=[vmem],
        out_specs=vmem,
        out_shape=jax.ShapeDtypeStruct(sent.shape, sent.dtype),
        scratch_shapes=[pltpu.SemaphoreType.DMA((PLANES,)), pltpu.SemaphoreType.DMA((PLANES,))],
        compiler_params=params(collective_id=number, has_side_effects=True),
        name="exchange",
    )(sent)


def params(**more):
    return pltpu.CompilerParams(vmem_limit_bytes=60 << 20, **more)


def whole(*shape):
    return pl.BlockSpec(shape, lambda *_: (0,) * len(shape))


def local(velocity, register, offsets, remesh_flag, keep_blocks):
    y_inv, x_inv, z_inv, z_fwd, x_fwd, y_fwd = tables()
    velocity = velocity.reshape(3, 2, MODES, NY)
    register = register.reshape(3, 2, MODES, NY)
    offsets = offsets.reshape(1, NY)
    remesh_flag = remesh_flag.reshape(1, NY)
    keep_blocks = keep_blocks.reshape(1, COLS)

    sent = pl.pallas_call(
        y_inverse_kernel,
        grid=(3,),
        in_specs=[
            pl.BlockSpec((1, 2, MODES, NY), lambda c: (c, 0, 0, 0)),
            whole(2, MY, 2 * NY),
        ],
        out_specs=pl.BlockSpec((DEVICES, PLANES, 1, 8, 128), lambda c: (0, 0, c, 0, 0)),
        out_shape=jax.ShapeDtypeStruct((DEVICES, PLANES, 3, 8, 128), BF16),
        scratch_shapes=[pltpu.VMEM((MODES, 2 * NY), BF16), pltpu.VMEM((8 * DEVICES, 128), F32)],
        compiler_params=params(),
        name="y_inverse",
    )(velocity, y_inv)
    came = exchange(sent, 0)
    came = came.reshape(ROWS, COLS, PLANES, 3, 8, 128)

    sent = pl.pallas_call(
        middle_kernel,
        grid=(PLANES,),
        in_specs=[
            pl.BlockSpec((ROWS, COLS, 1, 3, 8, 128), lambda q: (0, 0, q, 0, 0, 0)),
            whole(NX, 2 * MX),
            whole(MZ, 512),
            whole(512, MZ),
            whole(2 * MX, NX),
        ],
        out_specs=pl.BlockSpec((ROWS, COLS, 1, PRODUCTS, 8, 128), lambda q: (0, 0, q, 0, 0, 0)),
        out_shape=jax.ShapeDtypeStruct((ROWS, COLS, PLANES, PRODUCTS, 8, 128), BF16),
        scratch_shapes=[
            pltpu.VMEM((3, 256, NX), BF16),
            pltpu.VMEM((3, 512, MX), BF16),
            pltpu.VMEM((PRODUCTS, 256, 2 * MX), BF16),
        ],
        compiler_params=params(),
        name="middle",
    )(came, x_inv, z_inv, z_fwd, x_fwd)
    sent = sent.reshape(DEVICES, PLANES, PRODUCTS, 8, 128)
    came = exchange(sent, 1)

    vmem = pl.BlockSpec(memory_space=pltpu.VMEM)
    updated, packed = pl.pallas_call(
        update_kernel,
        in_specs=[vmem] * 6,
        out_specs=(vmem, vmem),
        out_shape=(
            jax.ShapeDtypeStruct((3, 2, MODES, NY), F32),
            jax.ShapeDtypeStruct((4, 6, 128, 128), BF16),
        ),
        scratch_shapes=[
            pltpu.VMEM((8 * DEVICES, 128), F32),
            pltpu.VMEM((PRODUCTS, 2 * MY, MODES), BF16),
            pltpu.VMEM((PRODUCTS, 2 * NY, 256), F32),
            pltpu.VMEM((6, NY, 256), F32),
        ],
        compiler_params=params(),
        name="update",
    )(came, y_fwd, velocity, register, offsets, remesh_flag)

    arrived = []
    for place, distance in enumerate(OFFSET_VALUES):
        route = [(i - distance, i) for i in range(COLS) if 0 <= i - distance < COLS]
        arrived.append(lax.ppermute(packed[place], "col", route))

    out = pl.pallas_call(
        remesh_kernel,
        in_specs=[vmem] * 8,
        out_specs=vmem,
        out_shape=jax.ShapeDtypeStruct((3, 2, MODES, NY), F32),
        compiler_params=params(),
        name="remesh",
    )(updated, *arrived, offsets, remesh_flag, keep_blocks)
    return out.reshape(3, 2, KZL, KXL, NY)


def solution(mesh):
    placed = (P(None, None, "row", "col", None), P(None, None, "row", "col", None), P(), P(), P())
    return jax.shard_map(
        local,
        mesh=mesh,
        in_specs=placed,
        out_specs=P(None, None, "row", "col", None),
        check_vma=False,
    )
```

```python
import math

import jax
import jax.numpy as jnp
import numpy as np
from jax import lax
from jax.experimental import pallas as pl
from jax.experimental.pallas import tpu as pltpu
from jax.sharding import PartitionSpec as P

NX, NY, NZ, NZH = 512, 256, 256, 128
MX, MY, MZ = 768, 384, 384
SHIFT_CAP = 32
ROWS, COLS = 8, 16
DEVICES = ROWS * COLS
PLANES = MY // DEVICES
KZL = NZH // ROWS
KXL = NX // COLS
MODES = KZL * KXL
PRODUCTS = 5

SHEAR_RATE = 40.0
SHEAR_TIME = 0.3
VISCOSITY = 0.0015
TIME_STEP = 0.008
REGISTER_WEIGHT = -153.0 / 128.0
UPDATE_WEIGHT = 8.0 / 15.0
OFFSET_VALUES = (-2, -1, 1, 2)
INVERSE_SCALE = 1.0 / math.sqrt(NX * NY * NZ)
FORWARD_SCALE = math.sqrt(NX * NY * NZ) / (MX * MY * MZ)

F32, BF16 = jnp.float32, jnp.bfloat16
NN = (((1,), (0,)), ((), ()))
NT = (((1,), (1,)), ((), ()))


def dot(a, b, dims=NN):
    return lax.dot_general(a, b, dims, preferred_element_type=F32)


def cos_sin(left, right, period):
    turns = np.mod(np.outer(left, right), period)
    angles = turns.astype(np.float32) * np.float32(2.0 * math.pi / period)
    return np.cos(angles), np.sin(angles)


def tables():
    kx = np.arange(NX) - NX // 2
    ky = np.arange(NY) - NY // 2
    quarter, row, four = np.meshgrid(np.arange(4), np.arange(ROWS), np.arange(4), indexing="ij")
    kz = (row * KZL + four * 4 + quarter).reshape(-1)

    def mixed(re, im, axis):
        out = np.stack([re, im], axis=axis + 1)
        shape = list(re.shape)
        shape[axis] *= 2
        return out.reshape(shape)

    c, s = cos_sin(np.arange(MY), ky, MY)
    y_inv = np.stack([np.concatenate([c, -s], 1), np.concatenate([s, c], 1)])
    y_inv = y_inv.reshape(2, PLANES, DEVICES, 2 * NY).transpose(1, 0, 2, 3).reshape(PLANES, 2 * DEVICES, 2 * NY)
    c, s = cos_sin(kx, np.arange(MX), MX)
    x_inv = np.concatenate([c, s], 1)
    x_fwd = np.concatenate([c.T, s.T], 0)
    c, s = cos_sin(np.arange(MZ), kz, MZ)
    w = np.where(kz == 0, 1.0, 2.0).astype(np.float32)[None]
    z_inv = np.concatenate([mixed(w * c, -w * s, 1), mixed(-w * s, -w * c, 1)], 1)
    z_fwd = np.concatenate([mixed(c.T, -s.T, 0), mixed(-s.T, -c.T, 0)], 0)
    c, s = cos_sin(ky, np.arange(MY), MY)
    c = c.reshape(NY, PLANES, DEVICES)
    s = s.reshape(NY, PLANES, DEVICES)
    y_fwd = np.concatenate([np.stack([c, s], 2), np.stack([-s, c], 2)], 0)
    y_fwd = y_fwd.reshape(2 * NY, 2 * MY)
    return [t.astype(jnp.bfloat16) for t in (y_inv, x_inv, z_inv, z_fwd, x_fwd, y_fwd)]


def lane_blocks(parts):
    lane = lax.broadcasted_iota(jnp.int32, parts[0].shape, 1)
    low_half = lane < 64
    even = (lane // 32) % 2 == 0
    a, b, c, d = parts
    roll = lambda x, n: pltpu.roll(x, n, 1)
    a, c = jnp.where(low_half, a, roll(c, 64)), jnp.where(low_half, roll(a, 64), c)
    b, d = jnp.where(low_half, b, roll(d, 64)), jnp.where(low_half, roll(b, 64), d)
    a, b = jnp.where(even, a, roll(b, 32)), jnp.where(even, roll(a, 96), b)
    c, d = jnp.where(even, c, roll(d, 32)), jnp.where(even, roll(c, 96), d)
    return a, b, c, d


def placing_matrix(moved):
    line = lax.broadcasted_iota(jnp.int32, (128, NY), 0)
    which = line // SHIFT_CAP
    value = jnp.where(which < 2, which - 2, which - 1)
    marked = jnp.broadcast_to(moved, (128, NY)) == value
    upto = lax.broadcasted_iota(jnp.int32, (NY, NY), 0) <= lax.broadcasted_iota(jnp.int32, (NY, NY), 1)
    rank = dot(jnp.where(marked, 1.0, 0.0).astype(BF16), jnp.where(upto, 1.0, 0.0).astype(BF16))
    slot = (line % SHIFT_CAP + 1).astype(F32)
    return jnp.where(marked & (rank == slot), 1.0, 0.0).astype(BF16)


def waves_of(kx, ky, kz):
    k1 = kx - SHEAR_TIME * ky
    squared = k1 * k1 + ky * ky + kz * kz
    return k1, squared, 1.0 / jnp.maximum(squared, 1.0)


def step_kernel(*refs):
    (v_any, r_any, yi_any, xi_any, zi_any, zf_any, xf_any, yf_any, off_ref, flag_ref, out_ref) = refs[:11]
    (v_ref, r_ref, yi_ref, xi_ref, zi_ref, zf_ref, xf_ref, yf_ref) = refs[11:19]
    (both, grids, send_b, recv_b, lines, waves, modes, send_c, recv_c) = refs[19:28]
    (points, partial, spectra, rates, packs, arrived) = refs[28:34]
    (load_sem, out_b, in_b, out_c, in_c, out_m, in_m) = refs[34:]

    loads = [
        pltpu.make_async_copy(source, target, load_sem.at[k])
        for k, (source, target) in enumerate(
            [
                (yi_any, yi_ref),
                (v_any, v_ref),
                (xi_any, xi_ref),
                (zi_any, zi_ref),
                (zf_any, zf_ref),
                (xf_any, xf_ref),
                (yf_any, yf_ref),
                (r_any, r_ref),
            ]
        )
    ]
    for load in loads:
        load.start()

    row, col = lax.axis_index("row"), lax.axis_index("col")
    me = row * COLS + col
    x, core, y, z = row // 2, lax.rem(row, 2), col // 4, lax.rem(col, 4)
    to_rows = [lax.rem(x + d, 4) * 2 + lax.rem(core + e, 2) for d in range(4) for e in range(2)]

    def all_peers(work):
        def step(t, carry):
            to_col = lax.rem(y + t // 4, 4) * 4 + lax.rem(z + lax.rem(t, 4), 4)
            for to_row in to_rows:
                work(to_row, to_col)
            return carry

        lax.fori_loop(1, COLS, step, 0)
        for to_row in to_rows[1:]:
            work(to_row, col)

    barrier = pltpu.get_barrier_semaphore()
    all_peers(
        lambda to_row, to_col: pl.semaphore_signal(
            barrier, inc=1, device_id=(to_row, to_col), device_id_type=pl.DeviceIdType.MESH
        )
    )

    def push(source, target, out_sem, in_sem):
        def one(to_row, to_col):
            pltpu.make_async_remote_copy(
                src_ref=source.at[to_row * COLS + to_col],
                dst_ref=target.at[me],
                send_sem=out_sem,
                recv_sem=in_sem,
                device_id=(to_row, to_col),
                device_id_type=pl.DeviceIdType.MESH,
            ).start()

        all_peers(one)
        target[me] = source[me]

    def drain(buffer, sem):
        others = buffer.at[pl.ds(0, DEVICES - 1)]
        pltpu.make_async_copy(others, others, sem).wait()

    loads[0].wait()
    loads[1].wait()
    for c in range(3):
        both[c, :, :NY] = v_ref[c, 0].astype(BF16)
        both[c, :, NY:] = v_ref[c, 1].astype(BF16)
    for q in range(PLANES):
        for c in range(3):
            grid = grids.at[(3 * q + c) % 2]
            for h in range(2):
                part = dot(yi_ref[q], both[c, h * 256:(h + 1) * 256, :], NT)
                for k in range(2):
                    for s in range(2):
                        grid[pl.ds((2 * h + k) * 2 + s, DEVICES, stride=8), :] = part[
                            s * DEVICES:(s + 1) * DEVICES, k * 128:(k + 1) * 128
                        ]
            send_b[q, :, c] = grid[...].reshape(DEVICES, 8, 128).astype(BF16)
        if q == 0:
            pl.semaphore_wait(barrier, DEVICES - 1)
        push(send_b.at[q], recv_b.at[q], out_b.at[q], in_b.at[q])

    for load in loads[2:6]:
        load.wait()
    for q in range(PLANES):
        drain(recv_b.at[q], in_b.at[q])
        for c in range(3):
            for g in range(4):
                parts = [
                    jnp.concatenate(
                        [recv_b[q, r * COLS + 4 * g + k, c].astype(F32) for r in range(ROWS)], axis=0
                    )
                    for k in range(4)
                ]
                for k, part in enumerate(lane_blocks(parts)):
                    lines[c, k * 64:(k + 1) * 64, g * 128:(g + 1) * 128] = part.astype(BF16)
        for c in range(3):
            for half in range(2):
                waves[c, half * 256:(half + 1) * 256, :] = dot(
                    lines[c], xi_ref[:, half * MX:(half + 1) * MX]
                ).astype(BF16)
        for t in range(3):
            cols = slice(t * 256, (t + 1) * 256)
            f0, f1, f2 = [dot(zi_ref[...], waves[c, :, cols]) * INVERSE_SCALE for c in range(3)]
            products = (f0 * f0 - f1 * f1, f0 * f1, f0 * f2, f1 * f2, f2 * f2 - f1 * f1)
            for e, product in enumerate(products):
                pair = dot(zf_ref[...], product.astype(BF16)).astype(BF16)
                modes[e, :, cols] = pair[:256]
                modes[e, :, slice(MX + t * 256, MX + (t + 1) * 256)] = pair[256:]
        for e in range(PRODUCTS):
            back = dot(modes[e], xf_ref[...])
            for g in range(4):
                parts = [back[k * 64:(k + 1) * 64, g * 128:(g + 1) * 128] for k in range(4)]
                for k, part in enumerate(lane_blocks(parts)):
                    for r in range(ROWS):
                        send_c[q, r * COLS + 4 * g + k, e] = part[r * 8:(r + 1) * 8].astype(BF16)
        push(send_c.at[q], recv_c.at[q], out_c.at[q], in_c.at[q])

    loads[7].wait()
    loads[6].wait()
    row0 = row * KZL
    col0 = col * KXL - NX // 2

    def prepare(b, carry):
        n0 = pl.multiple_of(b * KXL, KXL)
        shape = (KXL, NY)
        ky = (lax.broadcasted_iota(jnp.int32, shape, 1) - NY // 2).astype(F32)
        kx = (lax.broadcasted_iota(jnp.int32, shape, 0) + col0).astype(F32)
        kz = (row0 + b).astype(F32)
        k1, squared, inv = waves_of(kx, ky, kz)
        lift = (2.0 * SHEAR_RATE * TIME_STEP) * ky * inv
        damp = (VISCOSITY * TIME_STEP) * squared
        for r in range(2):
            v0 = v_ref[0, r, pl.ds(n0, KXL), :]
            for m, k in enumerate((k1, ky, kz)):
                v = v_ref[m, r, pl.ds(n0, KXL), :]
                rate = k * lift * v0 - damp * v
                if m == 1:
                    rate = rate - (SHEAR_RATE * TIME_STEP) * v0
                rate = rate + REGISTER_WEIGHT * r_ref[m, r, pl.ds(n0, KXL), :]
                out_ref[m, r, pl.ds(n0, KXL), :] = v + UPDATE_WEIGHT * rate
        return carry

    lax.fori_loop(0, KZL, prepare, 0)
    moved = off_ref[...] * flag_ref[...]
    placing = placing_matrix(moved)
    stays = (moved == 0).astype(F32)

    for q in range(PLANES):
        drain(recv_c.at[q], in_c.at[q])
        for e in range(PRODUCTS):
            grid = grids.at[(PRODUCTS * q + e) % 2]
            grid[...] = recv_c[q, :, e].reshape(8 * DEVICES, 128).astype(F32)
            for j in range(4):
                for s in range(2):
                    points[e, (2 * q + s) * 128:(2 * q + s + 1) * 128, j * 128:(j + 1) * 128] = grid[
                        pl.ds(2 * j + s, DEVICES, stride=8), :
                    ].astype(BF16)
        if q == 1:
            for e in range(PRODUCTS):
                for h in range(2):
                    partial[h, e] = dot(yf_ref[:, :512], points[e, :512, h * 256:(h + 1) * 256])

    scale = UPDATE_WEIGHT * TIME_STEP * FORWARD_SCALE

    def remesh_copy(h, place):
        shift = OFFSET_VALUES[place]
        return pltpu.make_async_remote_copy(
            src_ref=packs.at[h, place],
            dst_ref=arrived.at[h, place],
            send_sem=out_m.at[h, place],
            recv_sem=in_m.at[h, place],
            device_id=(row, col + shift),
            device_id_type=pl.DeviceIdType.MESH,
        )

    def inside(position):
        return (position >= 0) & (position < COLS)

    for h in range(2):
        cols = slice(h * 256, (h + 1) * 256)
        for e in range(PRODUCTS):
            spectra[e] = partial[h, e] + dot(yf_ref[:, 512:], points[e, 512:, cols])

        def project(b, carry):
            y0 = pl.multiple_of(b * 16, 16)
            shape = (16, 256)
            ky = (lax.broadcasted_iota(jnp.int32, shape, 0) + (y0 - NY // 2)).astype(F32)
            n = lax.broadcasted_iota(jnp.int32, shape, 1)
            kx = (n % KXL + col0).astype(F32)
            kz = (n // KXL + (row0 + h * 8)).astype(F32)
            k1, squared, inv = waves_of(kx, ky, kz)
            for r in range(2):
                sign = scale if r == 0 else -scale
                s0, s1, s2, s3, s4 = [
                    spectra[e, pl.ds((1 - r) * NY + y0, 16), :] * sign for e in range(PRODUCTS)
                ]
                a0 = k1 * s0 + ky * s1 + kz * s2
                a1 = k1 * s1 + kz * s3
                a2 = k1 * s2 + ky * s3 + kz * s4
                div = (k1 * a0 + ky * a1 + kz * a2) * inv
                rates[r, pl.ds(y0, 16), :] = a0 - k1 * div
                rates[2 + r, pl.ds(y0, 16), :] = a1 - ky * div
                rates[4 + r, pl.ds(y0, 16), :] = a2 - kz * div
            return carry

        lax.fori_loop(0, NY // 16, project, 0)
        for m in range(3):
            for r in range(2):
                updated = out_ref[m, r, cols, :] + rates[2 * m + r].T
                out_ref[m, r, cols, :] = updated
                packed = dot(updated.astype(BF16), placing, NT)
                parts = [packed[k * 64:(k + 1) * 64] for k in range(4)]
                for k, part in enumerate(lane_blocks(parts)):
                    packs[h, k, 2 * m + r] = part.astype(BF16)
        for place, shift in enumerate(OFFSET_VALUES):

            @pl.when(inside(col + shift))
            def _():
                remesh_copy(h, place).start()

            @pl.when(jnp.logical_not(inside(col - shift)))
            def _():
                arrived[h, place] = jnp.zeros((6, 64, 128), BF16)

    for h in range(2):
        for place, shift in enumerate(OFFSET_VALUES):

            @pl.when(inside(col - shift))
            def _():
                remesh_copy(h, place).wait_recv()

        for m in range(3):
            for r in range(2):
                parts = lane_blocks([arrived[h, place, 2 * m + r].astype(F32) for place in range(4)])
                for k, part in enumerate(parts):
                    rows = slice(h * 256 + k * 64, h * 256 + (k + 1) * 64)
                    out_ref[m, r, rows, :] = out_ref[m, r, rows, :] * stays + dot(part.astype(BF16), placing)

    for q in range(PLANES):
        drain(send_b.at[q], out_b.at[q])
        drain(send_c.at[q], out_c.at[q])
    for h in range(2):
        for place, shift in enumerate(OFFSET_VALUES):

            @pl.when(inside(col + shift))
            def _():
                remesh_copy(h, place).wait_send()


def local(velocity, register, offsets, remesh_flag, keep_blocks):
    constants = tables()
    velocity = velocity.reshape(3, 2, MODES, NY)
    register = register.reshape(3, 2, MODES, NY)
    anywhere = pl.BlockSpec(memory_space=pl.ANY)
    vmem = pl.BlockSpec(memory_space=pltpu.VMEM)
    out = pl.pallas_call(
        step_kernel,
        in_specs=[anywhere] * 8 + [vmem] * 2,
        out_specs=vmem,
        out_shape=jax.ShapeDtypeStruct((3, 2, MODES, NY), F32),
        scratch_shapes=[
            pltpu.VMEM(velocity.shape, F32),
            pltpu.VMEM(register.shape, F32),
            *[pltpu.VMEM(t.shape, BF16) for t in constants],
            pltpu.VMEM((3, MODES, 2 * NY), BF16),
            pltpu.VMEM((2, 8 * DEVICES, 128), F32),
            pltpu.VMEM((PLANES, DEVICES, 3, 8, 128), BF16),
            pltpu.VMEM((PLANES, DEVICES, 3, 8, 128), BF16),
            pltpu.VMEM((3, 256, NX), BF16),
            pltpu.VMEM((3, 512, MX), BF16),
            pltpu.VMEM((PRODUCTS, 256, 2 * MX), BF16),
            pltpu.VMEM((PLANES, DEVICES, PRODUCTS, 8, 128), BF16),
            pltpu.VMEM((PLANES, DEVICES, PRODUCTS, 8, 128), BF16),
            pltpu.VMEM((PRODUCTS, 2 * MY, MODES), BF16),
            pltpu.VMEM((2, PRODUCTS, 2 * NY, 256), F32),
            pltpu.VMEM((PRODUCTS, 2 * NY, 256), F32),
            pltpu.VMEM((6, NY, 256), F32),
            pltpu.VMEM((2, 4, 6, 64, 128), BF16),
            pltpu.VMEM((2, 4, 6, 64, 128), BF16),
            pltpu.SemaphoreType.DMA((8,)),
            pltpu.SemaphoreType.DMA((PLANES,)),
            pltpu.SemaphoreType.DMA((PLANES,)),
            pltpu.SemaphoreType.DMA((PLANES,)),
            pltpu.SemaphoreType.DMA((PLANES,)),
            pltpu.SemaphoreType.DMA((2, 4)),
            pltpu.SemaphoreType.DMA((2, 4)),
        ],
        compiler_params=pltpu.CompilerParams(
            vmem_limit_bytes=63 << 20, collective_id=0, has_side_effects=True
        ),
        name="step",
    )(velocity, register, *constants, offsets.reshape(1, NY), remesh_flag.reshape(1, NY))
    block = jnp.arange(COLS, dtype=jnp.int32)
    keep = jnp.sum(jnp.where(block == lax.axis_index("col"), keep_blocks, 0)).astype(F32)
    return out.reshape(3, 2, KZL, KXL, NY) * keep


def solution(mesh):
    placed = (P(None, None, "row", "col", None), P(None, None, "row", "col", None), P(), P(), P())
    return jax.shard_map(
        local,
        mesh=mesh,
        in_specs=placed,
        out_specs=P(None, None, "row", "col", None),
        check_vma=False,
    )
```

```python
import math

import jax
import jax.numpy as jnp
import numpy as np
from jax import lax
from jax.experimental import pallas as pl
from jax.experimental.pallas import tpu as pltpu
from jax.sharding import PartitionSpec as P

NX, NY, NZ, NZH = 512, 256, 256, 128
MX, MY, MZ = 768, 384, 384
SHIFT_CAP = 32
VMEM_LIMIT = 52 << 20
ROWS, COLS = 8, 16
DEVICES = ROWS * COLS
PLANES = MY // DEVICES
KZL = NZH // ROWS
KXL = NX // COLS
MODES = KZL * KXL
PRODUCTS = 5

SHEAR_RATE = 40.0
SHEAR_TIME = 0.3
VISCOSITY = 0.0015
TIME_STEP = 0.008
REGISTER_WEIGHT = -153.0 / 128.0
UPDATE_WEIGHT = 8.0 / 15.0
OFFSET_VALUES = (-2, -1, 1, 2)
INVERSE_SCALE = 1.0 / math.sqrt(NX * NY * NZ)
FORWARD_SCALE = math.sqrt(NX * NY * NZ) / (MX * MY * MZ)

F32, BF16 = jnp.float32, jnp.bfloat16
NN = (((1,), (0,)), ((), ()))
NT = (((1,), (1,)), ((), ()))


def dot(a, b, dims=NN):
    return lax.dot_general(a, b, dims, preferred_element_type=F32)


def cos_sin(left, right, period):
    turns = np.mod(np.outer(left, right), period)
    angles = turns.astype(np.float32) * np.float32(2.0 * math.pi / period)
    return np.cos(angles), np.sin(angles)


def tables():
    kx = np.arange(NX) - NX // 2
    ky = np.arange(NY) - NY // 2
    quarter, row, four = np.meshgrid(np.arange(4), np.arange(ROWS), np.arange(4), indexing="ij")
    kz = (row * KZL + four * 4 + quarter).reshape(-1)

    def mixed(re, im, axis):
        out = np.stack([re, im], axis=axis + 1)
        shape = list(re.shape)
        shape[axis] *= 2
        return out.reshape(shape)

    c, s = cos_sin(np.arange(MY), ky, MY)
    y_inv = np.stack([np.concatenate([c, -s], 1), np.concatenate([s, c], 1)])
    y_inv = y_inv.reshape(2, PLANES, DEVICES, 2 * NY).transpose(1, 0, 2, 3).reshape(PLANES, 2 * DEVICES, 2 * NY)
    c, s = cos_sin(kx, np.arange(MX), MX)
    x_inv = np.concatenate([c, s], 1)
    x_fwd = np.concatenate([c.T, s.T], 0)
    c, s = cos_sin(np.arange(MZ), kz, MZ)
    w = np.where(kz == 0, 1.0, 2.0).astype(np.float32)[None]
    z_inv = np.concatenate([mixed(w * c, -w * s, 1), mixed(-w * s, -w * c, 1)], 1)
    z_fwd = np.concatenate([mixed(c.T, -s.T, 0), mixed(-s.T, -c.T, 0)], 0)
    c, s = cos_sin(ky, np.arange(MY), MY)
    c = c.reshape(NY, PLANES, DEVICES)
    s = s.reshape(NY, PLANES, DEVICES)
    y_fwd = np.concatenate([np.stack([c, s], 2), np.stack([-s, c], 2)], 0)
    y_fwd = y_fwd.reshape(2 * NY, 2 * MY)
    return [t.astype(jnp.bfloat16) for t in (y_inv, x_inv, z_inv, z_fwd, x_fwd, y_fwd)]


def peer_order():
    rng = np.random.RandomState(0)
    left = [(a, b, c, d) for a in range(4) for b in range(4) for c in range(4) for d in range(2)][1:]
    left = [left[k] for k in rng.permutation(len(left))]
    hops = np.array([[0, 0], [1, 0], [1, 1], [0, 1]], np.float64)
    total, order = np.zeros(6), []
    while left:
        tries = [total + np.concatenate([hops[d] for d in o[:3]]) for o in left[:24]]
        best = int(np.argmin([np.round(t.var(), 9) for t in tries]))
        total = tries[best]
        order.append(left.pop(best))
    return order


def lane_blocks(parts):
    lane = lax.broadcasted_iota(jnp.int32, parts[0].shape, 1)
    low_half = lane < 64
    even = (lane // 32) % 2 == 0
    a, b, c, d = parts
    roll = lambda x, n: pltpu.roll(x, n, 1)
    a, c = jnp.where(low_half, a, roll(c, 64)), jnp.where(low_half, roll(a, 64), c)
    b, d = jnp.where(low_half, b, roll(d, 64)), jnp.where(low_half, roll(b, 64), d)
    a, b = jnp.where(even, a, roll(b, 32)), jnp.where(even, roll(a, 96), b)
    c, d = jnp.where(even, c, roll(d, 32)), jnp.where(even, roll(c, 96), d)
    return a, b, c, d


def placing_matrix(moved):
    line = lax.broadcasted_iota(jnp.int32, (128, NY), 0)
    which = line // SHIFT_CAP
    value = jnp.where(which < 2, which - 2, which - 1)
    marked = jnp.broadcast_to(moved, (128, NY)) == value
    upto = lax.broadcasted_iota(jnp.int32, (NY, NY), 0) <= lax.broadcasted_iota(jnp.int32, (NY, NY), 1)
    rank = dot(jnp.where(marked, 1.0, 0.0).astype(BF16), jnp.where(upto, 1.0, 0.0).astype(BF16))
    slot = (line % SHIFT_CAP + 1).astype(F32)
    return jnp.where(marked & (rank == slot), 1.0, 0.0).astype(BF16)


def waves_of(kx, ky, kz):
    k1 = kx - SHEAR_TIME * ky
    squared = k1 * k1 + ky * ky + kz * kz
    return k1, squared, 1.0 / jnp.maximum(squared, 1.0)


def step_kernel(*refs):
    (v_any, r_any, yi_any, xi_any, zi_any, zf_any, xf_any, yf_any) = refs[:8]
    (off_any, flag_any, keep_any, out_ref) = refs[8:12]
    (v_ref, r_ref, yi_ref, xi_ref, zi_ref, zf_ref, xf_ref, yf_ref) = refs[12:20]
    (off_ref, flag_ref, keep_ref) = refs[20:23]
    (both, grids, send_b, recv_b, lines, waves, modes, send_c, recv_c) = refs[23:32]
    (points, partial, rates, packs, arrived) = refs[32:37]
    (load_sem, out_b, in_b, out_c, in_c, out_m, in_m) = refs[37:]

    pairs = [
        (yi_any, yi_ref),
        (v_any, v_ref),
        (xi_any, xi_ref),
        (zi_any, zi_ref),
        (zf_any, zf_ref),
        (xf_any, xf_ref),
        (yf_any, yf_ref),
        (r_any, r_ref),
        (off_any, off_ref),
        (flag_any, flag_ref),
        (keep_any, keep_ref),
    ]
    loads = [pltpu.make_async_copy(*pair, load_sem.at[k]) for k, pair in enumerate(pairs)]
    for load in loads[:2]:
        load.start()

    row, col = lax.axis_index("row"), lax.axis_index("col")
    me = row * COLS + col
    x, core, y, z = row // 2, lax.rem(row, 2), col // 4, lax.rem(col, 4)
    to_rows = [lax.rem(x + d, 4) * 2 + lax.rem(core + e, 2) for d in range(4) for e in range(2)]
    to_cols = [lax.rem(y + d, 4) * 4 + lax.rem(z + e, 4) for d in range(4) for e in range(4)]
    order = peer_order()

    def all_peers(work):
        for dx, dy, dz, dcore in order:
            work(to_rows[dx * 2 + dcore], to_cols[dy * 4 + dz])

    barrier = pltpu.get_barrier_semaphore()
    all_peers(
        lambda to_row, to_col: pl.semaphore_signal(
            barrier, inc=1, device_id=(to_row, to_col), device_id_type=pl.DeviceIdType.MESH
        )
    )

    def push(source, target, out_sem, in_sem):
        def one(to_row, to_col):
            pltpu.make_async_remote_copy(
                src_ref=source.at[to_row * COLS + to_col],
                dst_ref=target.at[me],
                send_sem=out_sem,
                recv_sem=in_sem,
                device_id=(to_row, to_col),
                device_id_type=pl.DeviceIdType.MESH,
            ).start()

        all_peers(one)
        target[me] = source[me]

    def drain(buffer, sem):
        others = buffer.at[pl.ds(0, DEVICES - 1)]
        pltpu.make_async_copy(others, others, sem).wait()

    for load in loads[2:]:
        load.start()
    loads[0].wait()
    loads[1].wait()
    for c in range(3):
        both[c, :, :NY] = v_ref[c, 0].astype(BF16)
        both[c, :, NY:] = v_ref[c, 1].astype(BF16)

    def y_inverse(q):
        for c in range(3):
            grid = grids.at[c % 2]
            for h in range(2):
                part = dot(yi_ref[q], both[c, h * 256:(h + 1) * 256, :], NT)
                for k in range(2):
                    for s in range(2):
                        grid[pl.ds((2 * h + k) * 2 + s, DEVICES, stride=8), :] = part[
                            s * DEVICES:(s + 1) * DEVICES, k * 128:(k + 1) * 128
                        ]
            send_b[q, :, c] = grid[...].reshape(DEVICES, 8, 128).astype(BF16)

    y_inverse(0)
    pl.semaphore_wait(barrier, DEVICES - 1)

    def outward(q, carry):
        @pl.when(q > 0)
        def _():
            y_inverse(q)

        push(send_b.at[q], recv_b.at[q], out_b.at[q], in_b.at[q])
        return carry

    lax.fori_loop(0, PLANES, outward, 0)

    for load in loads[2:6]:
        load.wait()

    def middle(q, carry):
        drain(recv_b.at[q], in_b.at[q])
        for c in range(3):
            for g in range(4):
                parts = [
                    jnp.concatenate(
                        [recv_b[q, r * COLS + 4 * g + k, c].astype(F32) for r in range(ROWS)], axis=0
                    )
                    for k in range(4)
                ]
                for k, part in enumerate(lane_blocks(parts)):
                    lines[c, k * 64:(k + 1) * 64, g * 128:(g + 1) * 128] = part.astype(BF16)
        for c in range(3):
            for half in range(2):
                waves[c, half * 256:(half + 1) * 256, :] = dot(
                    lines[c], xi_ref[:, half * MX:(half + 1) * MX]
                ).astype(BF16)
        for t in range(3):
            cols = slice(t * 256, (t + 1) * 256)
            f0, f1, f2 = [dot(zi_ref[...], waves[c, :, cols]) * INVERSE_SCALE for c in range(3)]
            products = (f0 * f0 - f1 * f1, f0 * f1, f0 * f2, f1 * f2, f2 * f2 - f1 * f1)
            for e, product in enumerate(products):
                pair = dot(zf_ref[...], product.astype(BF16)).astype(BF16)
                modes[e, :, cols] = pair[:256]
                modes[e, :, slice(MX + t * 256, MX + (t + 1) * 256)] = pair[256:]
        for e in range(PRODUCTS):
            back = dot(modes[e], xf_ref[...])
            for g in range(4):
                parts = [back[k * 64:(k + 1) * 64, g * 128:(g + 1) * 128] for k in range(4)]
                for k, part in enumerate(lane_blocks(parts)):
                    for r in range(ROWS):
                        send_c[q, r * COLS + 4 * g + k, e] = part[r * 8:(r + 1) * 8].astype(BF16)
        push(send_c.at[q], recv_c.at[q], out_c.at[q], in_c.at[q])
        return carry

    lax.fori_loop(0, PLANES, middle, 0)

    for load in loads[6:]:
        load.wait()
    row0 = row * KZL
    col0 = col * KXL - NX // 2

    def prepare(b, carry):
        n0 = pl.multiple_of(b * KXL, KXL)
        shape = (KXL, NY)
        ky = (lax.broadcasted_iota(jnp.int32, shape, 1) - NY // 2).astype(F32)
        kx = (lax.broadcasted_iota(jnp.int32, shape, 0) + col0).astype(F32)
        kz = (row0 + b).astype(F32)
        k1, squared, inv = waves_of(kx, ky, kz)
        lift = (2.0 * SHEAR_RATE * TIME_STEP) * ky * inv
        damp = (VISCOSITY * TIME_STEP) * squared
        for r in range(2):
            v0 = v_ref[0, r, pl.ds(n0, KXL), :]
            for m, k in enumerate((k1, ky, kz)):
                v = v_ref[m, r, pl.ds(n0, KXL), :]
                rate = k * lift * v0 - damp * v
                if m == 1:
                    rate = rate - (SHEAR_RATE * TIME_STEP) * v0
                rate = rate + REGISTER_WEIGHT * r_ref[m, r, pl.ds(n0, KXL), :]
                out_ref[m, r, pl.ds(n0, KXL), :] = v + UPDATE_WEIGHT * rate
        return carry

    lax.fori_loop(0, KZL, prepare, 0)
    moved = off_ref[...] * flag_ref[...]
    placing = placing_matrix(moved)
    block = lax.broadcasted_iota(jnp.int32, (1, COLS), 1)
    keep = jnp.sum(jnp.where(block == col, keep_ref[...], 0).astype(F32), axis=1, keepdims=True)
    stays = (moved == 0).astype(F32) * keep

    def gather(q):
        drain(recv_c.at[q], in_c.at[q])
        for e in range(PRODUCTS):
            grid = grids.at[e % 2]
            grid[...] = recv_c[q, :, e].reshape(8 * DEVICES, 128).astype(F32)
            for j in range(4):
                for s in range(2):
                    points[q, e, s * 128:(s + 1) * 128, j * 128:(j + 1) * 128] = grid[
                        pl.ds(2 * j + s, DEVICES, stride=8), :
                    ].astype(BF16)


    def early(q, carry):
        gather(q)
        return carry

    lax.fori_loop(0, PLANES - 1, early, 0)
    for e in range(PRODUCTS):
        for h in range(2):
            cols = slice(h * 256, (h + 1) * 256)
            partial[h, e] = dot(yf_ref[:, :256], points[0, e, :, cols]) + dot(
                yf_ref[:, 256:512], points[1, e, :, cols]
            )
    gather(PLANES - 1)

    scale = UPDATE_WEIGHT * TIME_STEP * FORWARD_SCALE

    def remesh_copy(w, place):
        shift = OFFSET_VALUES[place]
        return pltpu.make_async_remote_copy(
            src_ref=packs.at[w, place],
            dst_ref=arrived.at[w, place],
            send_sem=out_m.at[w, place],
            recv_sem=in_m.at[w, place],
            device_id=(row, col + shift),
            device_id_type=pl.DeviceIdType.MESH,
        )

    def inside(position):
        return (position >= 0) & (position < COLS)

    for w in range(4):
        h, u = w // 2, w % 2
        if u == 0:
            for e in range(PRODUCTS):
                partial[h, e] += dot(yf_ref[:, 512:], points[2, e, :, h * 256:(h + 1) * 256])

        def project(b, carry):
            y0 = pl.multiple_of(b * 32, 32)
            shape = (32, 128)
            ky = (lax.broadcasted_iota(jnp.int32, shape, 0) + (y0 - NY // 2)).astype(F32)
            n = lax.broadcasted_iota(jnp.int32, shape, 1)
            kx = (n % KXL + col0).astype(F32)
            kz = (n // KXL + (row0 + w * 4)).astype(F32)
            k1, squared, inv = waves_of(kx, ky, kz)
            for r in range(2):
                sign = scale if r == 0 else -scale
                s0, s1, s2, s3, s4 = [
                    partial[h, e, pl.ds((1 - r) * NY + y0, 32), u * 128:(u + 1) * 128] * sign
                    for e in range(PRODUCTS)
                ]
                a0 = k1 * s0 + ky * s1 + kz * s2
                a1 = k1 * s1 + kz * s3
                a2 = k1 * s2 + ky * s3 + kz * s4
                div = (k1 * a0 + ky * a1 + kz * a2) * inv
                rates[r, pl.ds(y0, 32), :] = a0 - k1 * div
                rates[2 + r, pl.ds(y0, 32), :] = a1 - ky * div
                rates[4 + r, pl.ds(y0, 32), :] = a2 - kz * div
            return carry

        lax.fori_loop(0, NY // 32, project, 0)
        rows = slice(w * 128, (w + 1) * 128)
        for m in range(3):
            for r in range(2):
                updated = out_ref[m, r, rows, :] + rates[2 * m + r].T
                out_ref[m, r, rows, :] = updated * stays
                packed = dot(updated.astype(BF16), placing, NT)
                parts = [packed[k * 32:(k + 1) * 32] for k in range(4)]
                for k, part in enumerate(lane_blocks(parts)):
                    packs[w, k, 2 * m + r] = part.astype(BF16)
        for place, shift in enumerate(OFFSET_VALUES):

            @pl.when(inside(col + shift))
            def _():
                remesh_copy(w, place).start()

            @pl.when(jnp.logical_not(inside(col - shift)))
            def _():
                arrived[w, place] = jnp.zeros((6, 32, 128), BF16)

    for w in range(4):
        for place, shift in enumerate(OFFSET_VALUES):

            @pl.when(inside(col - shift))
            def _():
                remesh_copy(w, place).wait_recv()

        for m in range(3):
            for r in range(2):
                parts = lane_blocks([arrived[w, place, 2 * m + r].astype(F32) for place in range(4)])
                part = jnp.concatenate(parts, axis=0).astype(BF16)
                rows = slice(w * 128, (w + 1) * 128)
                out_ref[m, r, rows, :] += dot(part, placing) * keep

    for q in range(PLANES):
        drain(send_b.at[q], out_b.at[q])
        drain(send_c.at[q], out_c.at[q])
    for w in range(4):
        for place, shift in enumerate(OFFSET_VALUES):

            @pl.when(inside(col + shift))
            def _():
                remesh_copy(w, place).wait_send()


def local(velocity, register, offsets, remesh_flag, keep_blocks):
    constants = tables()
    velocity = velocity.reshape(3, 2, MODES, NY)
    register = register.reshape(3, 2, MODES, NY)
    anywhere = pl.BlockSpec(memory_space=pltpu.HBM)
    vmem = pl.BlockSpec(memory_space=pltpu.VMEM)
    out = pl.pallas_call(
        step_kernel,
        in_specs=[anywhere] * 11,
        out_specs=vmem,
        out_shape=pltpu.VMEM((3, 2, MODES, NY), F32),
        scratch_shapes=[
            pltpu.VMEM(velocity.shape, F32),
            pltpu.VMEM(register.shape, F32),
            *[pltpu.VMEM(t.shape, BF16) for t in constants],
            pltpu.VMEM((1, NY), jnp.int32),
            pltpu.VMEM((1, NY), jnp.int32),
            pltpu.VMEM((1, COLS), jnp.int32),
            pltpu.VMEM((3, MODES, 2 * NY), BF16),
            pltpu.VMEM((2, 8 * DEVICES, 128), F32),
            pltpu.VMEM((PLANES, DEVICES, 3, 8, 128), BF16),
            pltpu.VMEM((PLANES, DEVICES, 3, 8, 128), BF16),
            pltpu.VMEM((3, 256, NX), BF16),
            pltpu.VMEM((3, 512, MX), BF16),
            pltpu.VMEM((PRODUCTS, 256, 2 * MX), BF16),
            pltpu.VMEM((PLANES, DEVICES, PRODUCTS, 8, 128), BF16),
            pltpu.VMEM((PLANES, DEVICES, PRODUCTS, 8, 128), BF16),
            pltpu.VMEM((PLANES, PRODUCTS, 2 * DEVICES, MODES), BF16),
            pltpu.VMEM((2, PRODUCTS, 2 * NY, 256), F32),
            pltpu.VMEM((6, NY, 128), F32),
            pltpu.VMEM((4, 4, 6, 32, 128), BF16),
            pltpu.VMEM((4, 4, 6, 32, 128), BF16),
            pltpu.SemaphoreType.DMA((11,)),
            pltpu.SemaphoreType.DMA((PLANES,)),
            pltpu.SemaphoreType.DMA((PLANES,)),
            pltpu.SemaphoreType.DMA((PLANES,)),
            pltpu.SemaphoreType.DMA((PLANES,)),
            pltpu.SemaphoreType.DMA((4, 4)),
            pltpu.SemaphoreType.DMA((4, 4)),
        ],
        compiler_params=pltpu.CompilerParams(
            vmem_limit_bytes=VMEM_LIMIT, collective_id=0, has_side_effects=True
        ),
        name="step",
    )(
        velocity,
        register,
        *constants,
        offsets.reshape(1, NY),
        remesh_flag.reshape(1, NY),
        keep_blocks.reshape(1, COLS),
    )
    return out.reshape(3, 2, KZL, KXL, NY)


def solution(mesh):
    placed = (P(None, None, "row", "col", None), P(None, None, "row", "col", None), P(), P(), P())
    return jax.shard_map(
        local,
        mesh=mesh,
        in_specs=placed,
        out_specs=P(None, None, "row", "col", None),
        check_vma=False,
    )
```

```python
import math

import jax
import jax.numpy as jnp
import numpy as np
from jax import lax
from jax.experimental import pallas as pl
from jax.experimental.pallas import tpu as pltpu
from jax.sharding import PartitionSpec as P

NX, NY, NZ, NZH = 512, 256, 256, 128
MX, MY, MZ = 768, 384, 384
SHIFT_CAP = 32
VMEM_LIMIT = 52 << 20
ROWS, COLS = 8, 16
DEVICES = ROWS * COLS
PLANES = MY // DEVICES
KZL = NZH // ROWS
KXL = NX // COLS
MODES = KZL * KXL
PRODUCTS = 5
EARLY_TILES, LATE_TILES = (0, 3), (3, 2)

SHEAR_RATE = 40.0
SHEAR_TIME = 0.3
VISCOSITY = 0.0015
TIME_STEP = 0.008
REGISTER_WEIGHT = -153.0 / 128.0
UPDATE_WEIGHT = 8.0 / 15.0
OFFSET_VALUES = (-2, -1, 1, 2)
INVERSE_SCALE = 1.0 / math.sqrt(NX * NY * NZ)
FORWARD_SCALE = math.sqrt(NX * NY * NZ) / (MX * MY * MZ)

F32, BF16 = jnp.float32, jnp.bfloat16
NN = (((1,), (0,)), ((), ()))
NT = (((1,), (1,)), ((), ()))


def dot(a, b, dims=NN):
    return lax.dot_general(a, b, dims, preferred_element_type=F32)


def cos_sin(left, right, period):
    turns = np.mod(np.outer(left, right), period)
    angles = turns.astype(np.float32) * np.float32(2.0 * math.pi / period)
    return np.cos(angles), np.sin(angles)


def tables():
    kx = np.arange(NX) - NX // 2
    ky = np.arange(NY) - NY // 2
    quarter, row, four = np.meshgrid(np.arange(4), np.arange(ROWS), np.arange(4), indexing="ij")
    kz = (row * KZL + four * 4 + quarter).reshape(-1)

    def mixed(re, im, axis):
        out = np.stack([re, im], axis=axis + 1)
        shape = list(re.shape)
        shape[axis] *= 2
        return out.reshape(shape)

    c, s = cos_sin(np.arange(MY), ky, MY)
    y_inv = np.stack([np.concatenate([c, -s], 1), np.concatenate([s, c], 1)])
    y_inv = y_inv.reshape(2, PLANES, DEVICES, 2 * NY).transpose(1, 0, 2, 3).reshape(PLANES, 2 * DEVICES, 2 * NY)
    c, s = cos_sin(kx, np.arange(MX), MX)
    x_inv = np.concatenate([c, s], 1)
    x_fwd = np.concatenate([c.T, s.T], 0)
    c, s = cos_sin(np.arange(MZ), kz, MZ)
    w = np.where(kz == 0, 1.0, 2.0).astype(np.float32)[None]
    z_inv = np.concatenate([mixed(w * c, -w * s, 1), mixed(-w * s, -w * c, 1)], 1)
    z_fwd = np.concatenate([mixed(c.T, -s.T, 0), mixed(-s.T, -c.T, 0)], 0)
    swapped = z_fwd.reshape(64, 2, 4, MZ)[:, ::-1].reshape(512, MZ)
    z_fwd = np.stack([z_fwd, swapped])
    c, s = cos_sin(ky, np.arange(MY), MY)
    c = c.reshape(NY, PLANES, DEVICES)
    s = s.reshape(NY, PLANES, DEVICES)
    y_fwd = np.concatenate([np.stack([c, s], 2), np.stack([-s, c], 2)], 0)
    y_fwd = y_fwd.reshape(2 * NY, 2 * MY)
    return [t.astype(jnp.bfloat16) for t in (y_inv, x_inv, z_inv, z_fwd, x_fwd, y_fwd)]


def peer_order():
    rng = np.random.RandomState(0)
    left = [(a, b, c, d) for a in range(4) for b in range(4) for c in range(4) for d in range(2)][1:]
    left = [left[k] for k in rng.permutation(len(left))]
    hops = np.array([[0, 0], [1, 0], [1, 1], [0, 1]], np.float64)
    total, order = np.zeros(6), []
    while left:
        tries = [total + np.concatenate([hops[d] for d in o[:3]]) for o in left[:24]]
        best = int(np.argmin([np.round(t.var(), 9) for t in tries]))
        total = tries[best]
        order.append(left.pop(best))
    return order


def lane_blocks(parts):
    lane = lax.broadcasted_iota(jnp.int32, parts[0].shape, 1)
    low_half = lane < 64
    even = (lane // 32) % 2 == 0
    a, b, c, d = parts
    roll = lambda x, n: pltpu.roll(x, n, 1)
    a, c = jnp.where(low_half, a, roll(c, 64)), jnp.where(low_half, roll(a, 64), c)
    b, d = jnp.where(low_half, b, roll(d, 64)), jnp.where(low_half, roll(b, 64), d)
    a, b = jnp.where(even, a, roll(b, 32)), jnp.where(even, roll(a, 96), b)
    c, d = jnp.where(even, c, roll(d, 32)), jnp.where(even, roll(c, 96), d)
    return a, b, c, d


def placing_matrix(moved):
    line = lax.broadcasted_iota(jnp.int32, (128, NY), 0)
    which = line // SHIFT_CAP
    value = jnp.where(which < 2, which - 2, which - 1)
    marked = jnp.broadcast_to(moved, (128, NY)) == value
    upto = lax.broadcasted_iota(jnp.int32, (NY, NY), 0) <= lax.broadcasted_iota(jnp.int32, (NY, NY), 1)
    rank = dot(jnp.where(marked, 1.0, 0.0).astype(BF16), jnp.where(upto, 1.0, 0.0).astype(BF16))
    slot = (line % SHIFT_CAP + 1).astype(F32)
    return jnp.where(marked & (rank == slot), 1.0, 0.0).astype(BF16)


def waves_of(kx, ky, kz):
    k1 = kx - SHEAR_TIME * ky
    squared = k1 * k1 + ky * ky + kz * kz
    return k1, squared, 1.0 / jnp.maximum(squared, 1.0)


def step_kernel(*refs):
    (v_any, r_any, yi_any, xi_any, zi_any, zf_any, xf_any, yf_any) = refs[:8]
    (off_any, flag_any, keep_any, out_ref) = refs[8:12]
    (v_ref, r_ref, yi_ref, xi_ref, zi_ref, zf_ref, xf_ref, yf_ref) = refs[12:20]
    (off_ref, flag_ref, keep_ref) = refs[20:23]
    (both, grids, send_b, recv_b, lines, waves, modes, send_c, recv_c) = refs[23:32]
    (points, partial, rates, packs, arrived) = refs[32:37]
    (load_sem, out_b, in_b, out_c, in_c, out_m, in_m) = refs[37:]

    pairs = [
        (yi_any.at[0], yi_ref.at[0]),
        (v_any.at[0], v_ref.at[0]),
        (v_any.at[1], v_ref.at[1]),
        (v_any.at[2], v_ref.at[2]),
        (yi_any.at[pl.ds(1, 2)], yi_ref.at[pl.ds(1, 2)]),
        (xi_any, xi_ref),
        (zi_any, zi_ref),
        (zf_any, zf_ref),
        (xf_any, xf_ref),
        (yf_any, yf_ref),
        (r_any, r_ref),
        (off_any, off_ref),
        (flag_any, flag_ref),
        (keep_any, keep_ref),
    ]
    loads = [pltpu.make_async_copy(*pair, load_sem.at[k]) for k, pair in enumerate(pairs)]
    for load in loads[:5]:
        load.start()

    row, col = lax.axis_index("row"), lax.axis_index("col")
    me = row * COLS + col
    x, core, y, z = row // 2, lax.rem(row, 2), col // 4, lax.rem(col, 4)
    to_rows = [lax.rem(x + d, 4) * 2 + lax.rem(core + e, 2) for d in range(4) for e in range(2)]
    to_cols = [lax.rem(y + d, 4) * 4 + lax.rem(z + e, 4) for d in range(4) for e in range(4)]
    order = peer_order()

    def all_peers(work):
        for dx, dy, dz, dcore in order:
            work(to_rows[dx * 2 + dcore], to_cols[dy * 4 + dz])

    barrier = pltpu.get_barrier_semaphore()
    all_peers(
        lambda to_row, to_col: pl.semaphore_signal(
            barrier, inc=1, device_id=(to_row, to_col), device_id_type=pl.DeviceIdType.MESH
        )
    )

    def push(source, target, out_sem, in_sem, part=None):
        if part is not None:
            source = source.at[:, pl.ds(*part)]
            target = target.at[:, pl.ds(*part)]

        def one(to_row, to_col):
            pltpu.make_async_remote_copy(
                src_ref=source.at[to_row * COLS + to_col],
                dst_ref=target.at[me],
                send_sem=out_sem,
                recv_sem=in_sem,
                device_id=(to_row, to_col),
                device_id_type=pl.DeviceIdType.MESH,
            ).start()

        all_peers(one)
        target[me] = source[me]

    def drain(buffer, sem, part=None):
        if part is not None:
            buffer = buffer.at[:, pl.ds(*part)]
        others = buffer.at[pl.ds(0, DEVICES - 1)]
        pltpu.make_async_copy(others, others, sem).wait()

    for load in loads[5:]:
        load.start()
    def y_inverse(q, first=False):
        for c in range(3):
            if first:
                loads[1 + c].wait()
                both[c, :, :NY] = v_ref[c, 0].astype(BF16)
                both[c, :, NY:] = v_ref[c, 1].astype(BF16)
            grid = grids.at[c % 2]
            for h in range(2):
                part = dot(yi_ref[q], both[c, h * 256:(h + 1) * 256, :], NT)
                for k in range(2):
                    for s in range(2):
                        grid[pl.ds((2 * h + k) * 2 + s, DEVICES, stride=8), :] = part[
                            s * DEVICES:(s + 1) * DEVICES, k * 128:(k + 1) * 128
                        ]
            send_b[q, :, c] = grid[...].reshape(DEVICES, 8, 128).astype(BF16)

    loads[0].wait()
    y_inverse(0, first=True)
    loads[4].wait()
    pl.semaphore_wait(barrier, DEVICES - 1)

    def outward(q, carry):
        @pl.when(q > 0)
        def _():
            y_inverse(q)

        push(send_b.at[q], recv_b.at[q], out_b.at[q], in_b.at[q])
        return carry

    lax.fori_loop(0, PLANES, outward, 0)

    for load in loads[5:9]:
        load.wait()

    def middle(q, carry):
        drain(recv_b.at[q], in_b.at[q])
        for c in range(3):
            for g in range(4):
                parts = [
                    jnp.concatenate(
                        [recv_b[q, r * COLS + 4 * g + k, c].astype(F32) for r in range(ROWS)], axis=0
                    )
                    for k in range(4)
                ]
                for k, part in enumerate(lane_blocks(parts)):
                    lines[c, k * 64:(k + 1) * 64, g * 128:(g + 1) * 128] = part.astype(BF16)
        for c in range(3):
            for half in range(2):
                waves[c, half * 256:(half + 1) * 256, :] = dot(
                    lines[c], xi_ref[:, half * MX:(half + 1) * MX]
                ).astype(BF16)
        for t in range(3):
            cols = slice(t * 256, (t + 1) * 256)
            f0, f1, f2 = [dot(zi_ref[...], waves[c, :, cols]) * INVERSE_SCALE for c in range(3)]
            products = (f0 * f0 - f1 * f1, f0 * f1, f0 * f2, f1 * f2, f2 * f2 - f1 * f1)
            for e, product in enumerate(products):
                pair = dot(zf_ref[e % 2], product.astype(BF16)).astype(BF16)
                modes[e, :, cols] = pair[:256]
                modes[e, :, slice(MX + t * 256, MX + (t + 1) * 256)] = pair[256:]
        def returned(e, g):
            return lane_blocks(
                [back[e % 2][k * 64:(k + 1) * 64, g * 128:(g + 1) * 128] for k in range(4)]
            )

        def post(tile, device, part):
            for r in range(ROWS):
                send_c[q, r * COLS + device, tile] = part[r * 8:(r + 1) * 8].astype(BF16)

        for e in (0, 2):
            back = [dot(modes[e], xf_ref[...]), dot(modes[e + 1], xf_ref[...])]
            first = lax.broadcasted_iota(jnp.int32, (64, 128), 0) % 8 < 4
            for g in range(4):
                for k, (even, odd) in enumerate(zip(returned(0, g), returned(1, g))):
                    post(e // 2, 4 * g + k, jnp.where(first, even, odd))
                    post(3 + e // 2, 4 * g + k, jnp.where(first, odd, even))
        back = [dot(modes[4], xf_ref[...])]
        for g in range(4):
            for k, part in enumerate(returned(0, g)):
                post(2, 4 * g + k, part)

        @pl.when(q < PLANES - 1)
        def _():
            push(send_c.at[q], recv_c.at[q], out_c.at[q], in_c.at[q])

        @pl.when(q == PLANES - 1)
        def _():
            push(send_c.at[q], recv_c.at[q], out_c.at[q], in_c.at[q], EARLY_TILES)
            push(send_c.at[q], recv_c.at[q], out_c.at[q + 1], in_c.at[q + 1], LATE_TILES)

        return carry

    lax.fori_loop(0, PLANES, middle, 0)

    for load in loads[9:]:
        load.wait()
    row0 = row * KZL
    col0 = col * KXL - NX // 2

    def prepare(b, carry):
        n0 = pl.multiple_of(b * KXL, KXL)
        shape = (KXL, NY)
        ky = (lax.broadcasted_iota(jnp.int32, shape, 1) - NY // 2).astype(F32)
        kx = (lax.broadcasted_iota(jnp.int32, shape, 0) + col0).astype(F32)
        kz = (row0 + b).astype(F32)
        k1, squared, inv = waves_of(kx, ky, kz)
        lift = (2.0 * SHEAR_RATE * TIME_STEP) * ky * inv
        damp = (VISCOSITY * TIME_STEP) * squared
        for r in range(2):
            v0 = v_ref[0, r, pl.ds(n0, KXL), :]
            for m, k in enumerate((k1, ky, kz)):
                v = v_ref[m, r, pl.ds(n0, KXL), :]
                rate = k * lift * v0 - damp * v
                if m == 1:
                    rate = rate - (SHEAR_RATE * TIME_STEP) * v0
                rate = rate + REGISTER_WEIGHT * r_ref[m, r, pl.ds(n0, KXL), :]
                out_ref[m, r, pl.ds(n0, KXL), :] = v + UPDATE_WEIGHT * rate
        return carry

    lax.fori_loop(0, KZL, prepare, 0)
    moved = off_ref[...] * flag_ref[...]
    placing = placing_matrix(moved)
    block = lax.broadcasted_iota(jnp.int32, (1, COLS), 1)
    keep = jnp.sum(jnp.where(block == col, keep_ref[...], 0).astype(F32), axis=1, keepdims=True)
    stays = (moved == 0).astype(F32) * keep

    def tile_row(tile, r):
        if tile == 2:
            return 4, r // 2, r % 2
        half, low = tile // 3, r // 4
        return 2 * (tile % 3) + (low ^ half), 2 * half + r % 4 // 2, r % 2

    def gather(q, tiles):
        for tile in tiles:
            grid = grids.at[tile % 2]
            grid[...] = recv_c[q, :, tile].reshape(8 * DEVICES, 128).astype(F32)
            for r in range(8):
                e, j, s = tile_row(tile, r)
                points[q, e, s * 128:(s + 1) * 128, j * 128:(j + 1) * 128] = grid[
                    pl.ds(r, DEVICES, stride=8), :
                ].astype(BF16)


    def early(q, carry):
        drain(recv_c.at[q], in_c.at[q])
        gather(q, range(PRODUCTS))
        return carry

    lax.fori_loop(0, PLANES - 1, early, 0)
    for e in range(PRODUCTS):
        for h in range(2):
            cols = slice(h * 256, (h + 1) * 256)
            partial[h, e] = dot(yf_ref[:, :256], points[0, e, :, cols]) + dot(
                yf_ref[:, 256:512], points[1, e, :, cols]
            )
    scale = UPDATE_WEIGHT * TIME_STEP * FORWARD_SCALE

    def remesh_copy(w, place):
        shift = OFFSET_VALUES[place]
        return pltpu.make_async_remote_copy(
            src_ref=packs.at[w, place],
            dst_ref=arrived.at[w, place],
            send_sem=out_m.at[w, place],
            recv_sem=in_m.at[w, place],
            device_id=(row, col + shift),
            device_id_type=pl.DeviceIdType.MESH,
        )

    def inside(position):
        return (position >= 0) & (position < COLS)

    for w in range(4):
        h, u = w // 2, w % 2
        if u == 0:
            part = (EARLY_TILES, LATE_TILES)[h]
            drain(recv_c.at[PLANES - 1], in_c.at[PLANES - 1 + h], part)
            gather(PLANES - 1, range(part[0], part[0] + part[1]))
            for e in range(PRODUCTS):
                partial[h, e] += dot(yf_ref[:, 512:], points[2, e, :, h * 256:(h + 1) * 256])

        def project(b, carry):
            y0 = pl.multiple_of(b * 32, 32)
            shape = (32, 128)
            ky = (lax.broadcasted_iota(jnp.int32, shape, 0) + (y0 - NY // 2)).astype(F32)
            n = lax.broadcasted_iota(jnp.int32, shape, 1)
            kx = (n % KXL + col0).astype(F32)
            kz = (n // KXL + (row0 + w * 4)).astype(F32)
            k1, squared, inv = waves_of(kx, ky, kz)
            for r in range(2):
                sign = scale if r == 0 else -scale
                s0, s1, s2, s3, s4 = [
                    partial[h, e, pl.ds((1 - r) * NY + y0, 32), u * 128:(u + 1) * 128] * sign
                    for e in range(PRODUCTS)
                ]
                a0 = k1 * s0 + ky * s1 + kz * s2
                a1 = k1 * s1 + kz * s3
                a2 = k1 * s2 + ky * s3 + kz * s4
                div = (k1 * a0 + ky * a1 + kz * a2) * inv
                rates[r, pl.ds(y0, 32), :] = a0 - k1 * div
                rates[2 + r, pl.ds(y0, 32), :] = a1 - ky * div
                rates[4 + r, pl.ds(y0, 32), :] = a2 - kz * div
            return carry

        lax.fori_loop(0, NY // 32, project, 0)
        rows = slice(w * 128, (w + 1) * 128)
        for m in range(3):
            for r in range(2):
                updated = out_ref[m, r, rows, :] + rates[2 * m + r].T
                out_ref[m, r, rows, :] = updated * stays
                packed = dot(updated.astype(BF16), placing, NT)
                parts = [packed[k * 32:(k + 1) * 32] for k in range(4)]
                for k, part in enumerate(lane_blocks(parts)):
                    packs[w, k, 2 * m + r] = part.astype(BF16)
        for place, shift in enumerate(OFFSET_VALUES):

            @pl.when(inside(col + shift))
            def _():
                remesh_copy(w, place).start()

            @pl.when(jnp.logical_not(inside(col - shift)))
            def _():
                arrived[w, place] = jnp.zeros((6, 32, 128), BF16)

    for w in range(4):
        for place, shift in enumerate(OFFSET_VALUES):

            @pl.when(inside(col - shift))
            def _():
                remesh_copy(w, place).wait_recv()

        for m in range(3):
            for r in range(2):
                parts = lane_blocks([arrived[w, place, 2 * m + r].astype(F32) for place in range(4)])
                part = jnp.concatenate(parts, axis=0).astype(BF16)
                rows = slice(w * 128, (w + 1) * 128)
                out_ref[m, r, rows, :] += dot(part, placing) * keep

    for q in range(PLANES):
        drain(send_b.at[q], out_b.at[q])
        if q < PLANES - 1:
            drain(send_c.at[q], out_c.at[q])
    for h, part in enumerate((EARLY_TILES, LATE_TILES)):
        drain(send_c.at[PLANES - 1], out_c.at[PLANES - 1 + h], part)
    for w in range(4):
        for place, shift in enumerate(OFFSET_VALUES):

            @pl.when(inside(col + shift))
            def _():
                remesh_copy(w, place).wait_send()


def local(velocity, register, offsets, remesh_flag, keep_blocks):
    constants = tables()
    velocity = velocity.reshape(3, 2, MODES, NY)
    register = register.reshape(3, 2, MODES, NY)
    anywhere = pl.BlockSpec(memory_space=pltpu.HBM)
    vmem = pl.BlockSpec(memory_space=pltpu.VMEM)
    out = pl.pallas_call(
        step_kernel,
        in_specs=[anywhere] * 11,
        out_specs=vmem,
        out_shape=pltpu.VMEM((3, 2, MODES, NY), F32),
        scratch_shapes=[
            pltpu.VMEM(velocity.shape, F32),
            pltpu.VMEM(register.shape, F32),
            *[pltpu.VMEM(t.shape, BF16) for t in constants],
            pltpu.VMEM((1, NY), jnp.int32),
            pltpu.VMEM((1, NY), jnp.int32),
            pltpu.VMEM((1, COLS), jnp.int32),
            pltpu.VMEM((3, MODES, 2 * NY), BF16),
            pltpu.VMEM((2, 8 * DEVICES, 128), F32),
            pltpu.VMEM((PLANES, DEVICES, 3, 8, 128), BF16),
            pltpu.VMEM((PLANES, DEVICES, 3, 8, 128), BF16),
            pltpu.VMEM((3, 256, NX), BF16),
            pltpu.VMEM((3, 512, MX), BF16),
            pltpu.VMEM((PRODUCTS, 256, 2 * MX), BF16),
            pltpu.VMEM((PLANES, DEVICES, PRODUCTS, 8, 128), BF16),
            pltpu.VMEM((PLANES, DEVICES, PRODUCTS, 8, 128), BF16),
            pltpu.VMEM((PLANES, PRODUCTS, 2 * DEVICES, MODES), BF16),
            pltpu.VMEM((2, PRODUCTS, 2 * NY, 256), F32),
            pltpu.VMEM((6, NY, 128), F32),
            pltpu.VMEM((4, 4, 6, 32, 128), BF16),
            pltpu.VMEM((4, 4, 6, 32, 128), BF16),
            pltpu.SemaphoreType.DMA((14,)),
            pltpu.SemaphoreType.DMA((PLANES,)),
            pltpu.SemaphoreType.DMA((PLANES,)),
            pltpu.SemaphoreType.DMA((PLANES + 1,)),
            pltpu.SemaphoreType.DMA((PLANES + 1,)),
            pltpu.SemaphoreType.DMA((4, 4)),
            pltpu.SemaphoreType.DMA((4, 4)),
        ],
        compiler_params=pltpu.CompilerParams(
            vmem_limit_bytes=VMEM_LIMIT, collective_id=0, has_side_effects=True
        ),
        name="step",
    )(
        velocity,
        register,
        *constants,
        offsets.reshape(1, NY),
        remesh_flag.reshape(1, NY),
        keep_blocks.reshape(1, COLS),
    )
    return out.reshape(3, 2, KZL, KXL, NY)


def solution(mesh):
    placed = (P(None, None, "row", "col", None), P(None, None, "row", "col", None), P(), P(), P())
    return jax.shard_map(
        local,
        mesh=mesh,
        in_specs=placed,
        out_specs=P(None, None, "row", "col", None),
        check_vma=False,
    )
```

```python
import math

import jax
import jax.numpy as jnp
import numpy as np
from jax import lax
from jax.experimental import pallas as pl
from jax.experimental.pallas import tpu as pltpu
from jax.sharding import PartitionSpec as P

NX, NY, NZ, NZH = 512, 256, 256, 128
MX, MY, MZ = 768, 384, 384
SHIFT_CAP = 32
VMEM_LIMIT = 52 << 20
ROWS, COLS = 8, 16
DEVICES = ROWS * COLS
PLANES = MY // DEVICES
KZL = NZH // ROWS
KXL = NX // COLS
MODES = KZL * KXL
PRODUCTS = 5
EARLY_TILES, LATE_TILES = (0, 3), (3, 2)

SHEAR_RATE = 40.0
SHEAR_TIME = 0.3
VISCOSITY = 0.0015
TIME_STEP = 0.008
REGISTER_WEIGHT = -153.0 / 128.0
UPDATE_WEIGHT = 8.0 / 15.0
OFFSET_VALUES = (-2, -1, 1, 2)
INVERSE_SCALE = 1.0 / math.sqrt(NX * NY * NZ)
FORWARD_SCALE = math.sqrt(NX * NY * NZ) / (MX * MY * MZ)

F32, BF16 = jnp.float32, jnp.bfloat16
NN = (((1,), (0,)), ((), ()))
NT = (((1,), (1,)), ((), ()))


def dot(a, b, dims=NN):
    return lax.dot_general(a, b, dims, preferred_element_type=F32)


def cos_sin(left, right, period):
    turns = np.mod(np.outer(left, right), period)
    angles = turns.astype(np.float32) * np.float32(2.0 * math.pi / period)
    return np.cos(angles), np.sin(angles)


def tables():
    kx = np.arange(NX) - NX // 2
    ky = np.arange(NY) - NY // 2
    quarter, row, four = np.meshgrid(np.arange(4), np.arange(ROWS), np.arange(4), indexing="ij")
    kz = (row * KZL + four * 4 + quarter).reshape(-1)

    def mixed(re, im, axis):
        out = np.stack([re, im], axis=axis + 1)
        shape = list(re.shape)
        shape[axis] *= 2
        return out.reshape(shape)

    c, s = cos_sin(np.arange(MY), ky, MY)
    y_inv = np.stack([np.concatenate([c, -s], 1), np.concatenate([s, c], 1)])
    y_inv = y_inv.reshape(2, PLANES, DEVICES, 2 * NY).transpose(1, 0, 2, 3).reshape(PLANES, 2 * DEVICES, 2 * NY)
    c, s = cos_sin(kx, np.arange(MX), MX)
    x_inv = np.concatenate([c, s], 1)
    x_fwd = np.concatenate([c.T, s.T], 0)
    c, s = cos_sin(np.arange(MZ), kz, MZ)
    w = np.where(kz == 0, 1.0, 2.0).astype(np.float32)[None]
    z_inv = np.concatenate([mixed(w * c, -w * s, 1), mixed(-w * s, -w * c, 1)], 1)
    z_fwd = np.concatenate([mixed(c.T, -s.T, 0), mixed(-s.T, -c.T, 0)], 0)
    swapped = z_fwd.reshape(64, 2, 4, MZ)[:, ::-1].reshape(512, MZ)
    z_fwd = np.stack([z_fwd, swapped])
    c, s = cos_sin(ky, np.arange(MY), MY)
    c = c.reshape(NY, PLANES, DEVICES)
    s = s.reshape(NY, PLANES, DEVICES)
    y_fwd = np.concatenate([np.stack([c, s], 2), np.stack([-s, c], 2)], 0)
    y_fwd = y_fwd.reshape(2 * NY, 2 * MY)
    return [t.astype(jnp.bfloat16) for t in (y_inv, x_inv, z_inv, z_fwd, x_fwd, y_fwd)]


def peer_order():
    rng = np.random.RandomState(0)
    left = [(a, b, c, d) for a in range(4) for b in range(4) for c in range(4) for d in range(2)][1:]
    left = [left[k] for k in rng.permutation(len(left))]
    hops = np.array([[0, 0], [1, 0], [1, 1], [0, 1]], np.float64)
    total, order = np.zeros(6), []
    while left:
        tries = [total + np.concatenate([hops[d] for d in o[:3]]) for o in left[:24]]
        best = int(np.argmin([np.round(t.var(), 9) for t in tries]))
        total = tries[best]
        order.append(left.pop(best))
    return order


def lane_blocks(parts):
    lane = lax.broadcasted_iota(jnp.int32, parts[0].shape, 1)
    low_half = lane < 64
    even = (lane // 32) % 2 == 0
    a, b, c, d = parts
    roll = lambda x, n: pltpu.roll(x, n, 1)
    a, c = jnp.where(low_half, a, roll(c, 64)), jnp.where(low_half, roll(a, 64), c)
    b, d = jnp.where(low_half, b, roll(d, 64)), jnp.where(low_half, roll(b, 64), d)
    a, b = jnp.where(even, a, roll(b, 32)), jnp.where(even, roll(a, 96), b)
    c, d = jnp.where(even, c, roll(d, 32)), jnp.where(even, roll(c, 96), d)
    return a, b, c, d


def placing_matrix(moved):
    line = lax.broadcasted_iota(jnp.int32, (128, NY), 0)
    which = line // SHIFT_CAP
    value = jnp.where(which < 2, which - 2, which - 1)
    marked = jnp.broadcast_to(moved, (128, NY)) == value
    upto = lax.broadcasted_iota(jnp.int32, (NY, NY), 0) <= lax.broadcasted_iota(jnp.int32, (NY, NY), 1)
    rank = dot(jnp.where(marked, 1.0, 0.0).astype(BF16), jnp.where(upto, 1.0, 0.0).astype(BF16))
    slot = (line % SHIFT_CAP + 1).astype(F32)
    return jnp.where(marked & (rank == slot), 1.0, 0.0).astype(BF16)


def waves_of(kx, ky, kz):
    k1 = kx - SHEAR_TIME * ky
    squared = k1 * k1 + ky * ky + kz * kz
    return k1, squared, 1.0 / jnp.maximum(squared, 1.0)


def step_kernel(*refs):
    (v_any, r_any, yi_any, xi_any, zi_any, zf_any, xf_any, yf_any) = refs[:8]
    (off_any, flag_any, keep_any, out_ref) = refs[8:12]
    (v_ref, r_ref, yi_ref, xi_ref, zi_ref, zf_ref, xf_ref, yf_ref) = refs[12:20]
    (off_ref, flag_ref, keep_ref) = refs[20:23]
    (both, grids, send_b, recv_b, lines, waves, modes, send_c, recv_c) = refs[23:32]
    (points, partial, rates, packs, arrived) = refs[32:37]
    (load_sem, out_b, in_b, out_c, in_c, out_m, in_m) = refs[37:]

    pairs = [
        (yi_any.at[0], yi_ref.at[0]),
        (v_any.at[0], v_ref.at[0]),
        (v_any.at[1], v_ref.at[1]),
        (v_any.at[2], v_ref.at[2]),
        (yi_any.at[pl.ds(1, 2)], yi_ref.at[pl.ds(1, 2)]),
        (xi_any, xi_ref),
        (zi_any, zi_ref),
        (zf_any, zf_ref),
        (xf_any, xf_ref),
        (yf_any, yf_ref),
        (r_any, r_ref),
        (off_any, off_ref),
        (flag_any, flag_ref),
        (keep_any, keep_ref),
    ]
    loads = [pltpu.make_async_copy(*pair, load_sem.at[k]) for k, pair in enumerate(pairs)]
    for load in loads[:5]:
        load.start()

    row, col = lax.axis_index("row"), lax.axis_index("col")
    me = row * COLS + col
    x, core, y, z = row // 2, lax.rem(row, 2), col // 4, lax.rem(col, 4)
    to_rows = [lax.rem(x + d, 4) * 2 + lax.rem(core + e, 2) for d in range(4) for e in range(2)]
    to_cols = [lax.rem(y + d, 4) * 4 + lax.rem(z + e, 4) for d in range(4) for e in range(4)]
    order = peer_order()

    far_first = sorted(order, key=lambda o: -sum((0, 1, 2, 1)[d] for d in o[:3]))

    def all_peers(work, peers=order):
        for dx, dy, dz, dcore in peers:
            work(to_rows[dx * 2 + dcore], to_cols[dy * 4 + dz])

    barrier = pltpu.get_barrier_semaphore()
    all_peers(
        lambda to_row, to_col: pl.semaphore_signal(
            barrier, inc=1, device_id=(to_row, to_col), device_id_type=pl.DeviceIdType.MESH
        ),
        far_first,
    )

    def push(source, target, out_sem, in_sem, part=None):
        if part is not None:
            source = source.at[:, pl.ds(*part)]
            target = target.at[:, pl.ds(*part)]

        def one(to_row, to_col):
            pltpu.make_async_remote_copy(
                src_ref=source.at[to_row * COLS + to_col],
                dst_ref=target.at[me],
                send_sem=out_sem,
                recv_sem=in_sem,
                device_id=(to_row, to_col),
                device_id_type=pl.DeviceIdType.MESH,
            ).start()

        all_peers(one)
        target[me] = source[me]

    def drain(buffer, sem, part=None):
        if part is not None:
            buffer = buffer.at[:, pl.ds(*part)]
        others = buffer.at[pl.ds(0, DEVICES - 1)]
        pltpu.make_async_copy(others, others, sem).wait()

    for load in loads[5:]:
        load.start()
    def y_inverse(q, first=False):
        for c in range(3):
            if first:
                loads[1 + c].wait()
                both[c, :, :NY] = v_ref[c, 0].astype(BF16)
                both[c, :, NY:] = v_ref[c, 1].astype(BF16)
            grid = grids.at[c % 2]
            for h in range(2):
                part = dot(yi_ref[q], both[c, h * 256:(h + 1) * 256, :], NT)
                for k in range(2):
                    for s in range(2):
                        grid[pl.ds((2 * h + k) * 2 + s, DEVICES, stride=8), :] = part[
                            s * DEVICES:(s + 1) * DEVICES, k * 128:(k + 1) * 128
                        ]
            send_b[q, :, c] = grid[...].reshape(DEVICES, 8, 128).astype(BF16)

    loads[0].wait()
    y_inverse(0, first=True)
    loads[4].wait()
    pl.semaphore_wait(barrier, DEVICES - 1)

    def outward(q, carry):
        @pl.when(q > 0)
        def _():
            y_inverse(q)

        push(send_b.at[q], recv_b.at[q], out_b.at[q], in_b.at[q])
        return carry

    lax.fori_loop(0, PLANES, outward, 0)

    for load in loads[5:9]:
        load.wait()

    def middle(q, carry):
        drain(recv_b.at[q], in_b.at[q])
        for c in range(3):
            for g in range(4):
                parts = [
                    jnp.concatenate(
                        [recv_b[q, r * COLS + 4 * g + k, c].astype(F32) for r in range(ROWS)], axis=0
                    )
                    for k in range(4)
                ]
                for k, part in enumerate(lane_blocks(parts)):
                    lines[c, k * 64:(k + 1) * 64, g * 128:(g + 1) * 128] = part.astype(BF16)
        for c in range(3):
            for half in range(2):
                waves[c, half * 256:(half + 1) * 256, :] = dot(
                    lines[c], xi_ref[:, half * MX:(half + 1) * MX]
                ).astype(BF16)
        for t in range(3):
            cols = slice(t * 256, (t + 1) * 256)
            f0, f1, f2 = [dot(zi_ref[...], waves[c, :, cols]) * INVERSE_SCALE for c in range(3)]
            products = (f0 * f0 - f1 * f1, f0 * f1, f0 * f2, f1 * f2, f2 * f2 - f1 * f1)
            for e, product in enumerate(products):
                pair = dot(zf_ref[e % 2], product.astype(BF16)).astype(BF16)
                modes[e, :, cols] = pair[:256]
                modes[e, :, slice(MX + t * 256, MX + (t + 1) * 256)] = pair[256:]
        def returned(e, g):
            return lane_blocks(
                [back[e % 2][k * 64:(k + 1) * 64, g * 128:(g + 1) * 128] for k in range(4)]
            )

        def post(tile, device, part):
            for r in range(ROWS):
                send_c[q, r * COLS + device, tile] = part[r * 8:(r + 1) * 8].astype(BF16)

        for e in (0, 2):
            back = [dot(modes[e], xf_ref[...]), dot(modes[e + 1], xf_ref[...])]
            first = lax.broadcasted_iota(jnp.int32, (64, 128), 0) % 8 < 4
            for g in range(4):
                for k, (even, odd) in enumerate(zip(returned(0, g), returned(1, g))):
                    post(e // 2, 4 * g + k, jnp.where(first, even, odd))
                    post(3 + e // 2, 4 * g + k, jnp.where(first, odd, even))
        back = [dot(modes[4], xf_ref[...])]
        for g in range(4):
            for k, part in enumerate(returned(0, g)):
                post(2, 4 * g + k, part)

        @pl.when(q < PLANES - 1)
        def _():
            push(send_c.at[q], recv_c.at[q], out_c.at[q], in_c.at[q])

        @pl.when(q == PLANES - 1)
        def _():
            push(send_c.at[q], recv_c.at[q], out_c.at[q], in_c.at[q], EARLY_TILES)
            push(send_c.at[q], recv_c.at[q], out_c.at[q + 1], in_c.at[q + 1], LATE_TILES)

        return carry

    lax.fori_loop(0, PLANES, middle, 0)

    for load in loads[9:]:
        load.wait()
    row0 = row * KZL
    col0 = col * KXL - NX // 2

    def prepare(b, carry):
        n0 = pl.multiple_of(b * KXL, KXL)
        shape = (KXL, NY)
        ky = (lax.broadcasted_iota(jnp.int32, shape, 1) - NY // 2).astype(F32)
        kx = (lax.broadcasted_iota(jnp.int32, shape, 0) + col0).astype(F32)
        kz = (row0 + b).astype(F32)
        k1, squared, inv = waves_of(kx, ky, kz)
        lift = (2.0 * SHEAR_RATE * TIME_STEP) * ky * inv
        damp = (VISCOSITY * TIME_STEP) * squared
        for r in range(2):
            v0 = v_ref[0, r, pl.ds(n0, KXL), :]
            for m, k in enumerate((k1, ky, kz)):
                v = v_ref[m, r, pl.ds(n0, KXL), :]
                rate = k * lift * v0 - damp * v
                if m == 1:
                    rate = rate - (SHEAR_RATE * TIME_STEP) * v0
                rate = rate + REGISTER_WEIGHT * r_ref[m, r, pl.ds(n0, KXL), :]
                out_ref[m, r, pl.ds(n0, KXL), :] = v + UPDATE_WEIGHT * rate
        return carry

    lax.fori_loop(0, KZL, prepare, 0)
    moved = off_ref[...] * flag_ref[...]
    placing = placing_matrix(moved)
    block = lax.broadcasted_iota(jnp.int32, (1, COLS), 1)
    keep = jnp.sum(jnp.where(block == col, keep_ref[...], 0).astype(F32), axis=1, keepdims=True)
    stays = (moved == 0).astype(F32) * keep

    def tile_row(tile, r):
        if tile == 2:
            return 4, r // 2, r % 2
        half, low = tile // 3, r // 4
        return 2 * (tile % 3) + (low ^ half), 2 * half + r % 4 // 2, r % 2

    def gather(q, tiles):
        for tile in tiles:
            grid = grids.at[tile % 2]
            grid[...] = recv_c[q, :, tile].reshape(8 * DEVICES, 128).astype(F32)
            for r in range(8):
                e, j, s = tile_row(tile, r)
                points[q, e, s * 128:(s + 1) * 128, j * 128:(j + 1) * 128] = grid[
                    pl.ds(r, DEVICES, stride=8), :
                ].astype(BF16)


    def early(q, carry):
        drain(recv_c.at[q], in_c.at[q])
        gather(q, range(PRODUCTS))
        return carry

    lax.fori_loop(0, PLANES - 1, early, 0)
    for e in range(PRODUCTS):
        for h in range(2):
            cols = slice(h * 256, (h + 1) * 256)
            partial[h, e] = dot(yf_ref[:, :256], points[0, e, :, cols]) + dot(
                yf_ref[:, 256:512], points[1, e, :, cols]
            )
    scale = UPDATE_WEIGHT * TIME_STEP * FORWARD_SCALE

    def remesh_copy(w, place):
        shift = OFFSET_VALUES[place]
        return pltpu.make_async_remote_copy(
            src_ref=packs.at[w, place],
            dst_ref=arrived.at[w, place],
            send_sem=out_m.at[w, place],
            recv_sem=in_m.at[w, place],
            device_id=(row, col + shift),
            device_id_type=pl.DeviceIdType.MESH,
        )

    def inside(position):
        return (position >= 0) & (position < COLS)

    for w in range(4):
        h, u = w // 2, w % 2
        if u == 0:
            part = (EARLY_TILES, LATE_TILES)[h]
            drain(recv_c.at[PLANES - 1], in_c.at[PLANES - 1 + h], part)
            gather(PLANES - 1, range(part[0], part[0] + part[1]))
            for e in range(PRODUCTS):
                partial[h, e] += dot(yf_ref[:, 512:], points[2, e, :, h * 256:(h + 1) * 256])

        def project(b, carry):
            y0 = pl.multiple_of(b * 32, 32)
            shape = (32, 128)
            ky = (lax.broadcasted_iota(jnp.int32, shape, 0) + (y0 - NY // 2)).astype(F32)
            n = lax.broadcasted_iota(jnp.int32, shape, 1)
            kx = (n % KXL + col0).astype(F32)
            kz = (n // KXL + (row0 + w * 4)).astype(F32)
            k1, squared, inv = waves_of(kx, ky, kz)
            for r in range(2):
                sign = scale if r == 0 else -scale
                s0, s1, s2, s3, s4 = [
                    partial[h, e, pl.ds((1 - r) * NY + y0, 32), u * 128:(u + 1) * 128] * sign
                    for e in range(PRODUCTS)
                ]
                a0 = k1 * s0 + ky * s1 + kz * s2
                a1 = k1 * s1 + kz * s3
                a2 = k1 * s2 + ky * s3 + kz * s4
                div = (k1 * a0 + ky * a1 + kz * a2) * inv
                rates[r, pl.ds(y0, 32), :] = a0 - k1 * div
                rates[2 + r, pl.ds(y0, 32), :] = a1 - ky * div
                rates[4 + r, pl.ds(y0, 32), :] = a2 - kz * div
            return carry

        lax.fori_loop(0, NY // 32, project, 0)
        rows = slice(w * 128, (w + 1) * 128)
        for m in range(3):
            for r in range(2):
                updated = out_ref[m, r, rows, :] + rates[2 * m + r].T
                out_ref[m, r, rows, :] = updated * stays
                packed = dot(updated.astype(BF16), placing, NT)
                parts = [packed[k * 32:(k + 1) * 32] for k in range(4)]
                for k, part in enumerate(lane_blocks(parts)):
                    packs[w, k, 2 * m + r] = part.astype(BF16)
        for place, shift in enumerate(OFFSET_VALUES):

            @pl.when(inside(col + shift))
            def _():
                remesh_copy(w, place).start()

            @pl.when(jnp.logical_not(inside(col - shift)))
            def _():
                arrived[w, place] = jnp.zeros((6, 32, 128), BF16)

    for w in range(4):
        for place, shift in enumerate(OFFSET_VALUES):

            @pl.when(inside(col - shift))
            def _():
                remesh_copy(w, place).wait_recv()

        for m in range(3):
            for r in range(2):
                parts = lane_blocks([arrived[w, place, 2 * m + r].astype(F32) for place in range(4)])
                part = jnp.concatenate(parts, axis=0).astype(BF16)
                rows = slice(w * 128, (w + 1) * 128)
                out_ref[m, r, rows, :] += dot(part, placing) * keep

    for q in range(PLANES):
        drain(send_b.at[q], out_b.at[q])
        if q < PLANES - 1:
            drain(send_c.at[q], out_c.at[q])
    for h, part in enumerate((EARLY_TILES, LATE_TILES)):
        drain(send_c.at[PLANES - 1], out_c.at[PLANES - 1 + h], part)
    for w in range(4):
        for place, shift in enumerate(OFFSET_VALUES):

            @pl.when(inside(col + shift))
            def _():
                remesh_copy(w, place).wait_send()


def local(velocity, register, offsets, remesh_flag, keep_blocks):
    constants = tables()
    velocity = velocity.reshape(3, 2, MODES, NY)
    register = register.reshape(3, 2, MODES, NY)
    anywhere = pl.BlockSpec(memory_space=pltpu.HBM)
    vmem = pl.BlockSpec(memory_space=pltpu.VMEM)
    out = pl.pallas_call(
        step_kernel,
        in_specs=[anywhere] * 11,
        out_specs=vmem,
        out_shape=pltpu.VMEM((3, 2, MODES, NY), F32),
        scratch_shapes=[
            pltpu.VMEM(velocity.shape, F32),
            pltpu.VMEM(register.shape, F32),
            *[pltpu.VMEM(t.shape, BF16) for t in constants],
            pltpu.VMEM((1, NY), jnp.int32),
            pltpu.VMEM((1, NY), jnp.int32),
            pltpu.VMEM((1, COLS), jnp.int32),
            pltpu.VMEM((3, MODES, 2 * NY), BF16),
            pltpu.VMEM((2, 8 * DEVICES, 128), F32),
            pltpu.VMEM((PLANES, DEVICES, 3, 8, 128), BF16),
            pltpu.VMEM((PLANES, DEVICES, 3, 8, 128), BF16),
            pltpu.VMEM((3, 256, NX), BF16),
            pltpu.VMEM((3, 512, MX), BF16),
            pltpu.VMEM((PRODUCTS, 256, 2 * MX), BF16),
            pltpu.VMEM((PLANES, DEVICES, PRODUCTS, 8, 128), BF16),
            pltpu.VMEM((PLANES, DEVICES, PRODUCTS, 8, 128), BF16),
            pltpu.VMEM((PLANES, PRODUCTS, 2 * DEVICES, MODES), BF16),
            pltpu.VMEM((2, PRODUCTS, 2 * NY, 256), F32),
            pltpu.VMEM((6, NY, 128), F32),
            pltpu.VMEM((4, 4, 6, 32, 128), BF16),
            pltpu.VMEM((4, 4, 6, 32, 128), BF16),
            pltpu.SemaphoreType.DMA((14,)),
            pltpu.SemaphoreType.DMA((PLANES,)),
            pltpu.SemaphoreType.DMA((PLANES,)),
            pltpu.SemaphoreType.DMA((PLANES + 1,)),
            pltpu.SemaphoreType.DMA((PLANES + 1,)),
            pltpu.SemaphoreType.DMA((4, 4)),
            pltpu.SemaphoreType.DMA((4, 4)),
        ],
        compiler_params=pltpu.CompilerParams(
            vmem_limit_bytes=VMEM_LIMIT, collective_id=0, has_side_effects=True
        ),
        name="step",
    )(
        velocity,
        register,
        *constants,
        offsets.reshape(1, NY),
        remesh_flag.reshape(1, NY),
        keep_blocks.reshape(1, COLS),
    )
    return out.reshape(3, 2, KZL, KXL, NY)


def solution(mesh):
    placed = (P(None, None, "row", "col", None), P(None, None, "row", "col", None), P(), P(), P())
    return jax.shard_map(
        local,
        mesh=mesh,
        in_specs=placed,
        out_specs=P(None, None, "row", "col", None),
        check_vma=False,
    )
```

```python
import math

import jax
import jax.numpy as jnp
import numpy as np
from jax import lax
from jax.experimental import pallas as pl
from jax.experimental.pallas import tpu as pltpu
from jax.sharding import PartitionSpec as P

NX, NY, NZ, NZH = 512, 256, 256, 128
MX, MY, MZ = 768, 384, 384
SHIFT_CAP = 32
VMEM_LIMIT = 52 << 20
ROWS, COLS = 8, 16
DEVICES = ROWS * COLS
PLANES = MY // DEVICES
KZL = NZH // ROWS
KXL = NX // COLS
MODES = KZL * KXL
PRODUCTS = 5
SENT = 4
EARLY_TILES, LATE_TILES = (0, 2), (2, 2)

SHEAR_RATE = 40.0
SHEAR_TIME = 0.3
VISCOSITY = 0.0015
TIME_STEP = 0.008
REGISTER_WEIGHT = -153.0 / 128.0
UPDATE_WEIGHT = 8.0 / 15.0
OFFSET_VALUES = (-2, -1, 1, 2)
INVERSE_SCALE = 1.0 / math.sqrt(NX * NY * NZ)
FORWARD_SCALE = math.sqrt(NX * NY * NZ) / (MX * MY * MZ)

F32, BF16 = jnp.float32, jnp.bfloat16
NN = (((1,), (0,)), ((), ()))
NT = (((1,), (1,)), ((), ()))


def dot(a, b, dims=NN):
    return lax.dot_general(a, b, dims, preferred_element_type=F32)


def cos_sin(left, right, period):
    turns = np.mod(np.outer(left, right), period)
    angles = turns.astype(np.float32) * np.float32(2.0 * math.pi / period)
    return np.cos(angles), np.sin(angles)


def tables():
    kx = np.arange(NX) - NX // 2
    ky = np.arange(NY) - NY // 2
    quarter, row, four = np.meshgrid(np.arange(4), np.arange(ROWS), np.arange(4), indexing="ij")
    kz = (row * KZL + four * 4 + quarter).reshape(-1)

    def mixed(re, im, axis):
        out = np.stack([re, im], axis=axis + 1)
        shape = list(re.shape)
        shape[axis] *= 2
        return out.reshape(shape)

    c, s = cos_sin(np.arange(MY), ky, MY)
    y_inv = np.stack([np.concatenate([c, -s], 1), np.concatenate([s, c], 1)])
    y_inv = y_inv.reshape(2, PLANES, DEVICES, 2 * NY).transpose(1, 0, 2, 3).reshape(PLANES, 2 * DEVICES, 2 * NY)
    c, s = cos_sin(kx, np.arange(MX), MX)
    x_inv = np.concatenate([c, s], 1)
    x_fwd = np.concatenate([c.T, s.T], 0)
    c, s = cos_sin(np.arange(MZ), kz, MZ)
    w = np.where(kz == 0, 1.0, 2.0).astype(np.float32)[None]
    z_inv = np.concatenate([mixed(w * c, -w * s, 1), mixed(-w * s, -w * c, 1)], 1)
    z_fwd = np.concatenate([mixed(c.T, -s.T, 0), mixed(-s.T, -c.T, 0)], 0)
    c, s = cos_sin(ky, np.arange(MY), MY)
    c = c.reshape(NY, PLANES, DEVICES)
    s = s.reshape(NY, PLANES, DEVICES)
    y_fwd = np.concatenate([np.stack([c, s], 2), np.stack([-s, c], 2)], 0)
    y_fwd = y_fwd.reshape(2 * NY, 2 * MY)
    return [t.astype(jnp.bfloat16) for t in (y_inv, x_inv, z_inv, z_fwd, x_fwd, y_fwd)]


def peer_order():
    rng = np.random.RandomState(0)
    left = [(a, b, c, d) for a in range(4) for b in range(4) for c in range(4) for d in range(2)][1:]
    left = [left[k] for k in rng.permutation(len(left))]
    hops = np.array([[0, 0], [1, 0], [1, 1], [0, 1]], np.float64)
    total, order = np.zeros(6), []
    while left:
        tries = [total + np.concatenate([hops[d] for d in o[:3]]) for o in left[:24]]
        best = int(np.argmin([np.round(t.var(), 9) for t in tries]))
        total = tries[best]
        order.append(left.pop(best))
    return order


def lane_blocks(parts):
    lane = lax.broadcasted_iota(jnp.int32, parts[0].shape, 1)
    low_half = lane < 64
    even = (lane // 32) % 2 == 0
    a, b, c, d = parts
    roll = lambda x, n: pltpu.roll(x, n, 1)
    a, c = jnp.where(low_half, a, roll(c, 64)), jnp.where(low_half, roll(a, 64), c)
    b, d = jnp.where(low_half, b, roll(d, 64)), jnp.where(low_half, roll(b, 64), d)
    a, b = jnp.where(even, a, roll(b, 32)), jnp.where(even, roll(a, 96), b)
    c, d = jnp.where(even, c, roll(d, 32)), jnp.where(even, roll(c, 96), d)
    return a, b, c, d


NORM = 1.0 + SHEAR_TIME * SHEAR_TIME


def combine(back, k, g):
    t11, t12, t13, t23, t33 = [
        back[e, k * 64:(k + 1) * 64, g * 128:(g + 1) * 128] for e in range(PRODUCTS)
    ]
    shape = (64, 128)
    line = lax.broadcasted_iota(jnp.int32, shape, 0)
    kz = (line // 8 * KZL + line % 8 // 2 * 4 + k).astype(F32)
    kx = (lax.broadcasted_iota(jnp.int32, shape, 1) + (g * 128 - NX // 2)).astype(F32)
    a1 = kx * t11 + kz * t13
    a2 = kx * t12 + kz * t23
    a3 = kx * t13 + kz * t33
    b1 = t12 - SHEAR_TIME * t11
    b2 = -SHEAR_TIME * t12
    b3 = t23 - SHEAR_TIME * t13
    q1 = kx * a3 - kz * (a1 + SHEAR_TIME * a2)
    q2 = kx * b3 - kz * (b1 + SHEAR_TIME * b2)
    d = b2 - SHEAR_TIME * b1
    beta = NORM * (kx * a1 + kz * a3) - (kx * kx + kz * kz) * d
    gamma = NORM * (a2 - SHEAR_TIME * a1) + SHEAR_TIME * kx * d
    if k == 0 and g == 2:
        mean = (kx == 0.0) & (kz == 0.0)
        q1, q2, beta = jnp.where(mean, b1, q1), jnp.where(mean, b2, q2), jnp.where(mean, b3, beta)
    return q1, q2, beta, gamma


def placing_matrix(moved):
    line = lax.broadcasted_iota(jnp.int32, (128, NY), 0)
    which = line // SHIFT_CAP
    value = jnp.where(which < 2, which - 2, which - 1)
    marked = jnp.broadcast_to(moved, (128, NY)) == value
    upto = lax.broadcasted_iota(jnp.int32, (NY, NY), 0) <= lax.broadcasted_iota(jnp.int32, (NY, NY), 1)
    rank = dot(jnp.where(marked, 1.0, 0.0).astype(BF16), jnp.where(upto, 1.0, 0.0).astype(BF16))
    slot = (line % SHIFT_CAP + 1).astype(F32)
    return jnp.where(marked & (rank == slot), 1.0, 0.0).astype(BF16)


def waves_of(kx, ky, kz):
    k1 = kx - SHEAR_TIME * ky
    squared = k1 * k1 + ky * ky + kz * kz
    return k1, squared, 1.0 / jnp.maximum(squared, 1.0)


def step_kernel(*refs):
    (v_any, r_any, yi_any, xi_any, zi_any, zf_any, xf_any, yf_any) = refs[:8]
    (off_any, flag_any, keep_any, out_ref) = refs[8:12]
    (v_ref, r_ref, yi_ref, xi_ref, zi_ref, zf_ref, xf_ref, yf_ref) = refs[12:20]
    (off_ref, flag_ref, keep_ref) = refs[20:23]
    (both, grids, send_b, recv_b, lines, waves, modes, send_c, recv_c) = refs[23:32]
    (points, partial, back, rates, packs, arrived) = refs[32:38]
    (load_sem, out_b, in_b, out_c, in_c, out_m, in_m) = refs[38:]

    pairs = [
        (yi_any.at[0], yi_ref.at[0]),
        (v_any.at[0], v_ref.at[0]),
        (v_any.at[1], v_ref.at[1]),
        (v_any.at[2], v_ref.at[2]),
        (yi_any.at[pl.ds(1, 2)], yi_ref.at[pl.ds(1, 2)]),
        (xi_any, xi_ref),
        (zi_any, zi_ref),
        (zf_any, zf_ref),
        (xf_any, xf_ref),
        (yf_any, yf_ref),
        (r_any, r_ref),
        (off_any, off_ref),
        (flag_any, flag_ref),
        (keep_any, keep_ref),
    ]
    loads = [pltpu.make_async_copy(*pair, load_sem.at[k]) for k, pair in enumerate(pairs)]
    for load in loads[:5]:
        load.start()

    row, col = lax.axis_index("row"), lax.axis_index("col")
    me = row * COLS + col
    x, core, y, z = row // 2, lax.rem(row, 2), col // 4, lax.rem(col, 4)
    to_rows = [lax.rem(x + d, 4) * 2 + lax.rem(core + e, 2) for d in range(4) for e in range(2)]
    to_cols = [lax.rem(y + d, 4) * 4 + lax.rem(z + e, 4) for d in range(4) for e in range(4)]
    order = peer_order()

    far_first = sorted(order, key=lambda o: -sum((0, 1, 2, 1)[d] for d in o[:3]))

    def all_peers(work, peers=order):
        for dx, dy, dz, dcore in peers:
            work(to_rows[dx * 2 + dcore], to_cols[dy * 4 + dz])

    barrier = pltpu.get_barrier_semaphore()
    all_peers(
        lambda to_row, to_col: pl.semaphore_signal(
            barrier, inc=1, device_id=(to_row, to_col), device_id_type=pl.DeviceIdType.MESH
        ),
        far_first,
    )

    def push(source, target, out_sem, in_sem, part=None):
        if part is not None:
            source = source.at[:, pl.ds(*part)]
            target = target.at[:, pl.ds(*part)]

        def one(to_row, to_col):
            pltpu.make_async_remote_copy(
                src_ref=source.at[to_row * COLS + to_col],
                dst_ref=target.at[me],
                send_sem=out_sem,
                recv_sem=in_sem,
                device_id=(to_row, to_col),
                device_id_type=pl.DeviceIdType.MESH,
            ).start()

        all_peers(one)
        target[me] = source[me]

    def drain(buffer, sem, part=None):
        if part is not None:
            buffer = buffer.at[:, pl.ds(*part)]
        others = buffer.at[pl.ds(0, DEVICES - 1)]
        pltpu.make_async_copy(others, others, sem).wait()

    for load in loads[5:]:
        load.start()
    def y_inverse(q, first=False):
        for c in range(3):
            if first:
                loads[1 + c].wait()
                both[c, :, :NY] = v_ref[c, 0].astype(BF16)
                both[c, :, NY:] = v_ref[c, 1].astype(BF16)
            grid = grids.at[c % 2]
            for h in range(2):
                part = dot(yi_ref[q], both[c, h * 256:(h + 1) * 256, :], NT)
                for k in range(2):
                    for s in range(2):
                        grid[pl.ds((2 * h + k) * 2 + s, DEVICES, stride=8), :] = part[
                            s * DEVICES:(s + 1) * DEVICES, k * 128:(k + 1) * 128
                        ]
            send_b[q, :, c] = grid[...].reshape(DEVICES, 8, 128).astype(BF16)

    loads[0].wait()
    y_inverse(0, first=True)
    loads[4].wait()
    pl.semaphore_wait(barrier, DEVICES - 1)

    def outward(q, carry):
        @pl.when(q > 0)
        def _():
            y_inverse(q)

        push(send_b.at[q], recv_b.at[q], out_b.at[q], in_b.at[q])
        return carry

    lax.fori_loop(0, PLANES, outward, 0)

    for load in loads[5:9]:
        load.wait()

    def middle(q, carry):
        drain(recv_b.at[q], in_b.at[q])
        for c in range(3):
            for g in range(4):
                parts = [
                    jnp.concatenate(
                        [recv_b[q, r * COLS + 4 * g + k, c].astype(F32) for r in range(ROWS)], axis=0
                    )
                    for k in range(4)
                ]
                for k, part in enumerate(lane_blocks(parts)):
                    lines[c, k * 64:(k + 1) * 64, g * 128:(g + 1) * 128] = part.astype(BF16)
        for c in range(3):
            for half in range(2):
                waves[c, half * 256:(half + 1) * 256, :] = dot(
                    lines[c], xi_ref[:, half * MX:(half + 1) * MX]
                ).astype(BF16)
        for t in range(3):
            cols = slice(t * 256, (t + 1) * 256)
            f0, f1, f2 = [dot(zi_ref[...], waves[c, :, cols]) * INVERSE_SCALE for c in range(3)]
            products = (f0 * f0 - f1 * f1, f0 * f1, f0 * f2, f1 * f2, f2 * f2 - f1 * f1)
            for e, product in enumerate(products):
                pair = dot(zf_ref[...], product.astype(BF16)).astype(BF16)
                modes[e, :, cols] = pair[:256]
                modes[e, :, slice(MX + t * 256, MX + (t + 1) * 256)] = pair[256:]
        for e in range(PRODUCTS):
            back[e] = dot(modes[e], xf_ref[...])
        first = lax.broadcasted_iota(jnp.int32, (64, 128), 0) % 8 < 4
        for g in range(4):
            sums = [combine(back, k, g) for k in range(4)]
            for f in (0, 2):
                even = lane_blocks([sums[k][f] for k in range(4)])
                odd = lane_blocks([sums[k][f + 1] for k in range(4)])
                for k in range(4):
                    low = jnp.where(first, even[k], pltpu.roll(odd[k], 4, 0))
                    high = jnp.where(first, pltpu.roll(even[k], 60, 0), odd[k])
                    for tile, part in ((f // 2, low), (2 + f // 2, high)):
                        for r in range(ROWS):
                            send_c[q, r * COLS + 4 * g + k, tile] = part[r * 8:(r + 1) * 8].astype(BF16)

        @pl.when(q < PLANES - 1)
        def _():
            push(send_c.at[q], recv_c.at[q], out_c.at[q], in_c.at[q])

        @pl.when(q == PLANES - 1)
        def _():
            push(send_c.at[q], recv_c.at[q], out_c.at[q], in_c.at[q], EARLY_TILES)
            push(send_c.at[q], recv_c.at[q], out_c.at[q + 1], in_c.at[q + 1], LATE_TILES)

        return carry

    lax.fori_loop(0, PLANES, middle, 0)

    for load in loads[9:]:
        load.wait()
    row0 = row * KZL
    col0 = col * KXL - NX // 2

    def prepare(b, carry):
        n0 = pl.multiple_of(b * KXL, KXL)
        shape = (KXL, NY)
        ky = (lax.broadcasted_iota(jnp.int32, shape, 1) - NY // 2).astype(F32)
        kx = (lax.broadcasted_iota(jnp.int32, shape, 0) + col0).astype(F32)
        kz = (row0 + b).astype(F32)
        k1, squared, inv = waves_of(kx, ky, kz)
        lift = (2.0 * SHEAR_RATE * TIME_STEP) * ky * inv
        damp = (VISCOSITY * TIME_STEP) * squared
        for r in range(2):
            v0 = v_ref[0, r, pl.ds(n0, KXL), :]
            for m, k in enumerate((k1, ky, kz)):
                v = v_ref[m, r, pl.ds(n0, KXL), :]
                rate = k * lift * v0 - damp * v
                if m == 1:
                    rate = rate - (SHEAR_RATE * TIME_STEP) * v0
                rate = rate + REGISTER_WEIGHT * r_ref[m, r, pl.ds(n0, KXL), :]
                out_ref[m, r, pl.ds(n0, KXL), :] = v + UPDATE_WEIGHT * rate
        return carry

    lax.fori_loop(0, KZL, prepare, 0)
    moved = off_ref[...] * flag_ref[...]
    placing = placing_matrix(moved)
    block = lax.broadcasted_iota(jnp.int32, (1, COLS), 1)
    keep = jnp.sum(jnp.where(block == col, keep_ref[...], 0).astype(F32), axis=1, keepdims=True)
    stays = (moved == 0).astype(F32) * keep

    def tile_row(tile, r):
        return 2 * (tile % 2) + r // 4, 2 * (tile // 2) + r % 4 // 2, r % 2

    def gather(q, tiles):
        for tile in tiles:
            grid = grids.at[tile % 2]
            grid[...] = recv_c[q, :, tile].reshape(8 * DEVICES, 128).astype(F32)
            for r in range(8):
                e, j, s = tile_row(tile, r)
                points[q, e, s * 128:(s + 1) * 128, j * 128:(j + 1) * 128] = grid[
                    pl.ds(r, DEVICES, stride=8), :
                ].astype(BF16)


    def early(q, carry):
        drain(recv_c.at[q], in_c.at[q])
        gather(q, range(SENT))
        return carry

    lax.fori_loop(0, PLANES - 1, early, 0)
    for e in range(SENT):
        for h in range(2):
            cols = slice(h * 256, (h + 1) * 256)
            partial[h, e] = dot(yf_ref[:, :256], points[0, e, :, cols]) + dot(
                yf_ref[:, 256:512], points[1, e, :, cols]
            )
    scale = UPDATE_WEIGHT * TIME_STEP * FORWARD_SCALE

    def remesh_copy(w, place):
        shift = OFFSET_VALUES[place]
        return pltpu.make_async_remote_copy(
            src_ref=packs.at[w, place],
            dst_ref=arrived.at[w, place],
            send_sem=out_m.at[w, place],
            recv_sem=in_m.at[w, place],
            device_id=(row, col + shift),
            device_id_type=pl.DeviceIdType.MESH,
        )

    def inside(position):
        return (position >= 0) & (position < COLS)

    for w in range(4):
        h, u = w // 2, w % 2
        if u == 0:
            part = (EARLY_TILES, LATE_TILES)[h]
            drain(recv_c.at[PLANES - 1], in_c.at[PLANES - 1 + h], part)
            gather(PLANES - 1, range(part[0], part[0] + part[1]))
            for e in range(SENT):
                partial[h, e] += dot(yf_ref[:, 512:], points[2, e, :, h * 256:(h + 1) * 256])

        def project(b, carry):
            y0 = pl.multiple_of(b * 32, 32)
            shape = (32, 128)
            ky = (lax.broadcasted_iota(jnp.int32, shape, 0) + (y0 - NY // 2)).astype(F32)
            n = lax.broadcasted_iota(jnp.int32, shape, 1)
            kx = (n % KXL + col0).astype(F32)
            kz = (n // KXL + (row0 + w * 4)).astype(F32)
            k1, squared, inv = waves_of(kx, ky, kz)
            flat = kx * kx + kz * kz
            mean = flat == 0.0
            weight = scale / jnp.where(mean, 1.0, kx * kx + NORM * kz * kz)
            by_beta = (ky - (SHEAR_TIME / NORM) * kx) * inv * weight
            by_gamma = (ky * ky - flat * (1.0 / NORM)) * inv * weight
            c21 = ky * kx + SHEAR_TIME * kz * kz
            c22 = kz * kz + k1 * kx
            c23 = kz * (ky - SHEAR_TIME * k1)
            alone = jnp.where(mean, ky * scale, 0.0)
            for r in range(2):
                q1, q2, beta, gamma = [
                    partial[h, e, pl.ds((1 - r) * NY + y0, 32), u * 128:(u + 1) * 128] for e in range(SENT)
                ]
                p1 = (q1 + ky * q2) * weight
                p2 = by_beta * beta + by_gamma * gamma
                across = (q2 - SHEAR_TIME * q1) * (1.0 / NORM)
                n1 = c21 * p2 - kz * p1 + alone * (q1 + SHEAR_TIME * across)
                n2 = alone * (q2 - across) - c22 * p2 - SHEAR_TIME * kz * p1
                n3 = c23 * p2 + kx * p1 + alone * beta
                for m, part in enumerate((n1, n2, n3)):
                    rates[2 * m + r, pl.ds(y0, 32), :] = part if r == 0 else -part
            return carry

        lax.fori_loop(0, NY // 32, project, 0)
        rows = slice(w * 128, (w + 1) * 128)
        for m in range(3):
            for r in range(2):
                updated = out_ref[m, r, rows, :] + rates[2 * m + r].T
                out_ref[m, r, rows, :] = updated * stays
                packed = dot(updated.astype(BF16), placing, NT)
                parts = [packed[k * 32:(k + 1) * 32] for k in range(4)]
                for k, part in enumerate(lane_blocks(parts)):
                    packs[w, k, 2 * m + r] = part.astype(BF16)
        for place, shift in enumerate(OFFSET_VALUES):

            @pl.when(inside(col + shift))
            def _():
                remesh_copy(w, place).start()

            @pl.when(jnp.logical_not(inside(col - shift)))
            def _():
                arrived[w, place] = jnp.zeros((6, 32, 128), BF16)

    for w in range(4):
        for place, shift in enumerate(OFFSET_VALUES):

            @pl.when(inside(col - shift))
            def _():
                remesh_copy(w, place).wait_recv()

        for m in range(3):
            for r in range(2):
                parts = lane_blocks([arrived[w, place, 2 * m + r].astype(F32) for place in range(4)])
                part = jnp.concatenate(parts, axis=0).astype(BF16)
                rows = slice(w * 128, (w + 1) * 128)
                out_ref[m, r, rows, :] += dot(part, placing) * keep

    for q in range(PLANES):
        drain(send_b.at[q], out_b.at[q])
        if q < PLANES - 1:
            drain(send_c.at[q], out_c.at[q])
    for h, part in enumerate((EARLY_TILES, LATE_TILES)):
        drain(send_c.at[PLANES - 1], out_c.at[PLANES - 1 + h], part)
    for w in range(4):
        for place, shift in enumerate(OFFSET_VALUES):

            @pl.when(inside(col + shift))
            def _():
                remesh_copy(w, place).wait_send()


def local(velocity, register, offsets, remesh_flag, keep_blocks):
    constants = tables()
    velocity = velocity.reshape(3, 2, MODES, NY)
    register = register.reshape(3, 2, MODES, NY)
    anywhere = pl.BlockSpec(memory_space=pltpu.HBM)
    vmem = pl.BlockSpec(memory_space=pltpu.VMEM)
    out = pl.pallas_call(
        step_kernel,
        in_specs=[anywhere] * 11,
        out_specs=vmem,
        out_shape=pltpu.VMEM((3, 2, MODES, NY), F32),
        scratch_shapes=[
            pltpu.VMEM(velocity.shape, F32),
            pltpu.VMEM(register.shape, F32),
            *[pltpu.VMEM(t.shape, BF16) for t in constants],
            pltpu.VMEM((1, NY), jnp.int32),
            pltpu.VMEM((1, NY), jnp.int32),
            pltpu.VMEM((1, COLS), jnp.int32),
            pltpu.VMEM((3, MODES, 2 * NY), BF16),
            pltpu.VMEM((2, 8 * DEVICES, 128), F32),
            pltpu.VMEM((PLANES, DEVICES, 3, 8, 128), BF16),
            pltpu.VMEM((PLANES, DEVICES, 3, 8, 128), BF16),
            pltpu.VMEM((3, 256, NX), BF16),
            pltpu.VMEM((3, 512, MX), BF16),
            pltpu.VMEM((PRODUCTS, 256, 2 * MX), BF16),
            pltpu.VMEM((PLANES, DEVICES, SENT, 8, 128), BF16),
            pltpu.VMEM((PLANES, DEVICES, SENT, 8, 128), BF16),
            pltpu.VMEM((PLANES, SENT, 2 * DEVICES, MODES), BF16),
            pltpu.VMEM((2, SENT, 2 * NY, 256), F32),
            pltpu.VMEM((PRODUCTS, 256, NX), F32),
            pltpu.VMEM((6, NY, 128), F32),
            pltpu.VMEM((4, 4, 6, 32, 128), BF16),
            pltpu.VMEM((4, 4, 6, 32, 128), BF16),
            pltpu.SemaphoreType.DMA((14,)),
            pltpu.SemaphoreType.DMA((PLANES,)),
            pltpu.SemaphoreType.DMA((PLANES,)),
            pltpu.SemaphoreType.DMA((PLANES + 1,)),
            pltpu.SemaphoreType.DMA((PLANES + 1,)),
            pltpu.SemaphoreType.DMA((4, 4)),
            pltpu.SemaphoreType.DMA((4, 4)),
        ],
        compiler_params=pltpu.CompilerParams(
            vmem_limit_bytes=VMEM_LIMIT, collective_id=0, has_side_effects=True
        ),
        name="step",
    )(
        velocity,
        register,
        *constants,
        offsets.reshape(1, NY),
        remesh_flag.reshape(1, NY),
        keep_blocks.reshape(1, COLS),
    )
    return out.reshape(3, 2, KZL, KXL, NY)


def solution(mesh):
    placed = (P(None, None, "row", "col", None), P(None, None, "row", "col", None), P(), P(), P())
    return jax.shard_map(
        local,
        mesh=mesh,
        in_specs=placed,
        out_specs=P(None, None, "row", "col", None),
        check_vma=False,
    )
```

```python
import math

import jax
import jax.numpy as jnp
import numpy as np
from jax import lax
from jax.experimental import pallas as pl
from jax.experimental.pallas import tpu as pltpu
from jax.sharding import PartitionSpec as P

NX, NY, NZ, NZH = 512, 256, 256, 128
MX, MY, MZ = 768, 384, 384
SHIFT_CAP = 32
VMEM_LIMIT = 52 << 20
ROWS, COLS = 8, 16
DEVICES = ROWS * COLS
PLANES = MY // DEVICES
KZL = NZH // ROWS
KXL = NX // COLS
MODES = KZL * KXL
PRODUCTS = 5
SENT = 4
EARLY_TILES, LATE_TILES = (0, 2), (2, 2)

SHEAR_RATE = 40.0
SHEAR_TIME = 0.3
VISCOSITY = 0.0015
TIME_STEP = 0.008
REGISTER_WEIGHT = -153.0 / 128.0
UPDATE_WEIGHT = 8.0 / 15.0
OFFSET_VALUES = (-2, -1, 1, 2)
INVERSE_SCALE = 1.0 / math.sqrt(NX * NY * NZ)
FORWARD_SCALE = math.sqrt(NX * NY * NZ) / (MX * MY * MZ)

F32, BF16 = jnp.float32, jnp.bfloat16
NN = (((1,), (0,)), ((), ()))
NT = (((1,), (1,)), ((), ()))


def dot(a, b, dims=NN):
    return lax.dot_general(a, b, dims, preferred_element_type=F32)


def cos_sin(left, right, period):
    turns = np.mod(np.outer(left, right), period)
    angles = turns.astype(np.float32) * np.float32(2.0 * math.pi / period)
    return np.cos(angles), np.sin(angles)


def tables():
    kx = np.arange(NX) - NX // 2
    ky = np.arange(NY) - NY // 2
    quarter, row, four = np.meshgrid(np.arange(4), np.arange(ROWS), np.arange(4), indexing="ij")
    kz = (row * KZL + four * 4 + quarter).reshape(-1)

    def mixed(re, im, axis):
        out = np.stack([re, im], axis=axis + 1)
        shape = list(re.shape)
        shape[axis] *= 2
        return out.reshape(shape)

    c, s = cos_sin(np.arange(MY), ky, MY)
    y_inv = np.stack([np.concatenate([c, -s], 1), np.concatenate([s, c], 1)])
    y_inv = y_inv.reshape(2, PLANES, DEVICES, 2 * NY).transpose(1, 0, 2, 3).reshape(PLANES, 2 * DEVICES, 2 * NY)
    c, s = cos_sin(kx, np.arange(MX), MX)
    x_inv = np.concatenate([c, s], 1)
    x_fwd = np.concatenate([c.T, s.T], 0)
    c, s = cos_sin(np.arange(MZ), kz, MZ)
    w = np.where(kz == 0, 1.0, 2.0).astype(np.float32)[None]
    z_inv = np.concatenate([mixed(w * c, -w * s, 1), mixed(-w * s, -w * c, 1)], 1)
    z_fwd = np.concatenate([mixed(c.T, -s.T, 0), mixed(-s.T, -c.T, 0)], 0)
    c, s = cos_sin(ky, np.arange(MY), MY)
    c = c.reshape(NY, PLANES, DEVICES)
    s = s.reshape(NY, PLANES, DEVICES)
    y_fwd = np.concatenate([np.stack([c, s], 2), np.stack([-s, c], 2)], 0)
    y_fwd = y_fwd.reshape(2 * NY, 2 * MY)
    return [t.astype(jnp.bfloat16) for t in (y_inv, x_inv, z_inv, z_fwd, x_fwd, y_fwd)]


def peer_order():
    rng = np.random.RandomState(0)
    left = [(a, b, c, d) for a in range(4) for b in range(4) for c in range(4) for d in range(2)][1:]
    left = [left[k] for k in rng.permutation(len(left))]
    hops = np.array([[0, 0], [1, 0], [1, 1], [0, 1]], np.float64)
    total, order = np.zeros(6), []
    while left:
        tries = [total + np.concatenate([hops[d] for d in o[:3]]) for o in left[:24]]
        best = int(np.argmin([np.round(t.var(), 9) for t in tries]))
        total = tries[best]
        order.append(left.pop(best))
    return order


def lane_blocks(parts):
    lane = lax.broadcasted_iota(jnp.int32, parts[0].shape, 1)
    low_half = lane < 64
    even = (lane // 32) % 2 == 0
    a, b, c, d = parts
    roll = lambda x, n: pltpu.roll(x, n, 1)
    a, c = jnp.where(low_half, a, roll(c, 64)), jnp.where(low_half, roll(a, 64), c)
    b, d = jnp.where(low_half, b, roll(d, 64)), jnp.where(low_half, roll(b, 64), d)
    a, b = jnp.where(even, a, roll(b, 32)), jnp.where(even, roll(a, 96), b)
    c, d = jnp.where(even, c, roll(d, 32)), jnp.where(even, roll(c, 96), d)
    return a, b, c, d


NORM = 1.0 + SHEAR_TIME * SHEAR_TIME


def combine(back, k, g):
    t11, t12, t13, t23, t33 = [
        back[e, k * 64:(k + 1) * 64, g * 128:(g + 1) * 128] for e in range(PRODUCTS)
    ]
    shape = (64, 128)
    line = lax.broadcasted_iota(jnp.int32, shape, 0)
    kz = (line // 8 * KZL + line % 8 // 2 * 4 + k).astype(F32)
    kx = (lax.broadcasted_iota(jnp.int32, shape, 1) + (g * 128 - NX // 2)).astype(F32)
    a1 = kx * t11 + kz * t13
    a2 = kx * t12 + kz * t23
    a3 = kx * t13 + kz * t33
    b1 = t12 - SHEAR_TIME * t11
    b2 = -SHEAR_TIME * t12
    b3 = t23 - SHEAR_TIME * t13
    q1 = kx * a3 - kz * (a1 + SHEAR_TIME * a2)
    q2 = kx * b3 - kz * (b1 + SHEAR_TIME * b2)
    d = b2 - SHEAR_TIME * b1
    beta = NORM * (kx * a1 + kz * a3) - (kx * kx + kz * kz) * d
    gamma = NORM * (a2 - SHEAR_TIME * a1) + SHEAR_TIME * kx * d
    if k == 0 and g == 2:
        mean = (kx == 0.0) & (kz == 0.0)
        q1, q2, beta = jnp.where(mean, b1, q1), jnp.where(mean, b2, q2), jnp.where(mean, b3, beta)
    return q1, q2, beta, gamma


def placing_matrix(moved):
    line = lax.broadcasted_iota(jnp.int32, (128, NY), 0)
    which = line // SHIFT_CAP
    value = jnp.where(which < 2, which - 2, which - 1)
    marked = jnp.broadcast_to(moved, (128, NY)) == value
    upto = lax.broadcasted_iota(jnp.int32, (NY, NY), 0) <= lax.broadcasted_iota(jnp.int32, (NY, NY), 1)
    rank = dot(jnp.where(marked, 1.0, 0.0).astype(BF16), jnp.where(upto, 1.0, 0.0).astype(BF16))
    slot = (line % SHIFT_CAP + 1).astype(F32)
    return jnp.where(marked & (rank == slot), 1.0, 0.0).astype(BF16)


def waves_of(kx, ky, kz):
    k1 = kx - SHEAR_TIME * ky
    squared = k1 * k1 + ky * ky + kz * kz
    return k1, squared, 1.0 / jnp.maximum(squared, 1.0)


def step_kernel(*refs):
    (v_any, r_any, yi_any, xi_any, zi_any, zf_any, xf_any, yf_any) = refs[:8]
    (off_any, flag_any, keep_any, out_ref) = refs[8:12]
    (v_ref, r_ref, yi_ref, xi_ref, zi_ref, zf_ref, xf_ref, yf_ref) = refs[12:20]
    (off_ref, flag_ref, keep_ref) = refs[20:23]
    (both, grids, send_b, recv_b, lines, waves, modes, send_c, recv_c) = refs[23:32]
    (points, partial, back, rates, packs, arrived) = refs[32:38]
    (load_sem, out_b, in_b, out_c, in_c, out_m, in_m) = refs[38:]

    pairs = [
        (yi_any.at[0], yi_ref.at[0]),
        (v_any.at[0], v_ref.at[0]),
        (v_any.at[1], v_ref.at[1]),
        (v_any.at[2], v_ref.at[2]),
        (yi_any.at[pl.ds(1, 2)], yi_ref.at[pl.ds(1, 2)]),
        (xi_any, xi_ref),
        (zi_any, zi_ref),
        (zf_any, zf_ref),
        (xf_any, xf_ref),
        (yf_any, yf_ref),
        (r_any, r_ref),
        (off_any, off_ref),
        (flag_any, flag_ref),
        (keep_any, keep_ref),
    ]
    loads = [pltpu.make_async_copy(*pair, load_sem.at[k]) for k, pair in enumerate(pairs)]
    for load in loads[:5]:
        load.start()

    row, col = lax.axis_index("row"), lax.axis_index("col")
    me = row * COLS + col
    x, core, y, z = row // 2, lax.rem(row, 2), col // 4, lax.rem(col, 4)
    to_rows = [lax.rem(x + d, 4) * 2 + lax.rem(core + e, 2) for d in range(4) for e in range(2)]
    to_cols = [lax.rem(y + d, 4) * 4 + lax.rem(z + e, 4) for d in range(4) for e in range(4)]
    order = peer_order()

    far_first = sorted(order, key=lambda o: -sum((0, 1, 2, 1)[d] for d in o[:3]))

    def all_peers(work, peers=order):
        for dx, dy, dz, dcore in peers:
            work(to_rows[dx * 2 + dcore], to_cols[dy * 4 + dz])

    barrier = pltpu.get_barrier_semaphore()
    all_peers(
        lambda to_row, to_col: pl.semaphore_signal(
            barrier, inc=1, device_id=(to_row, to_col), device_id_type=pl.DeviceIdType.MESH
        ),
        far_first,
    )

    def push(source, target, out_sem, in_sem, part=None):
        if part is not None:
            source = source.at[:, pl.ds(*part)]
            target = target.at[:, pl.ds(*part)]

        def one(to_row, to_col):
            pltpu.make_async_remote_copy(
                src_ref=source.at[to_row * COLS + to_col],
                dst_ref=target.at[me],
                send_sem=out_sem,
                recv_sem=in_sem,
                device_id=(to_row, to_col),
                device_id_type=pl.DeviceIdType.MESH,
            ).start()

        all_peers(one)
        target[me] = source[me]

    def drain(buffer, sem, part=None):
        if part is not None:
            buffer = buffer.at[:, pl.ds(*part)]
        others = buffer.at[pl.ds(0, DEVICES - 1)]
        pltpu.make_async_copy(others, others, sem).wait()

    for load in loads[5:]:
        load.start()
    def y_inverse(q, first=False):
        for c in range(3):
            if first:
                loads[1 + c].wait()
                both[c, :, :NY] = v_ref[c, 0].astype(BF16)
                both[c, :, NY:] = v_ref[c, 1].astype(BF16)
            grid = grids.at[c % 2]
            for h in range(2):
                part = dot(yi_ref[q], both[c, h * 256:(h + 1) * 256, :], NT)
                for k in range(2):
                    for s in range(2):
                        grid[pl.ds((2 * h + k) * 2 + s, DEVICES, stride=8), :] = part[
                            s * DEVICES:(s + 1) * DEVICES, k * 128:(k + 1) * 128
                        ]
            send_b[q, :, c] = grid[...].reshape(DEVICES, 8, 128).astype(BF16)

    loads[0].wait()
    y_inverse(0, first=True)
    loads[4].wait()
    pl.semaphore_wait(barrier, DEVICES - 1)

    def outward(q, carry):
        @pl.when(q > 0)
        def _():
            y_inverse(q)

        push(send_b.at[q], recv_b.at[q], out_b.at[q], in_b.at[q])
        return carry

    lax.fori_loop(0, PLANES, outward, 0)

    for load in loads[5:9]:
        load.wait()

    def middle(q, carry):
        drain(recv_b.at[q], in_b.at[q])
        for c in range(3):
            for g in range(4):
                parts = [
                    jnp.concatenate(
                        [recv_b[q, r * COLS + 4 * g + k, c].astype(F32) for r in range(ROWS)], axis=0
                    )
                    for k in range(4)
                ]
                for k, part in enumerate(lane_blocks(parts)):
                    lines[c, k * 64:(k + 1) * 64, g * 128:(g + 1) * 128] = part.astype(BF16)
        for c in range(3):
            for half in range(2):
                waves[c, half * 256:(half + 1) * 256, :] = dot(
                    lines[c], xi_ref[:, half * MX:(half + 1) * MX]
                ).astype(BF16)
        for t in range(3):
            cols = slice(t * 256, (t + 1) * 256)
            f0, f1, f2 = [dot(zi_ref[...], waves[c, :, cols]) * INVERSE_SCALE for c in range(3)]
            products = (f0 * f0 - f1 * f1, f0 * f1, f0 * f2, f1 * f2, f2 * f2 - f1 * f1)
            for e, product in enumerate(products):
                pair = dot(zf_ref[...], product.astype(BF16)).astype(BF16)
                modes[e, :, cols] = pair[:256]
                modes[e, :, slice(MX + t * 256, MX + (t + 1) * 256)] = pair[256:]
        for e in range(PRODUCTS):
            back[e] = dot(modes[e], xf_ref[...])
        first = lax.broadcasted_iota(jnp.int32, (64, 128), 0) % 8 < 4
        for g in range(4):
            sums = [combine(back, k, g) for k in range(4)]
            for f in (0, 2):
                even = lane_blocks([sums[k][f] for k in range(4)])
                odd = lane_blocks([sums[k][f + 1] for k in range(4)])
                for k in range(4):
                    low = jnp.where(first, even[k], pltpu.roll(odd[k], 4, 0))
                    high = jnp.where(first, pltpu.roll(even[k], 60, 0), odd[k])
                    for tile, part in ((f // 2, low), (2 + f // 2, high)):
                        for r in range(ROWS):
                            send_c[q, r * COLS + 4 * g + k, tile] = part[r * 8:(r + 1) * 8].astype(BF16)

        @pl.when(q < PLANES - 1)
        def _():
            push(send_c.at[q], recv_c.at[q], out_c.at[q], in_c.at[q])

        @pl.when(q == PLANES - 1)
        def _():
            push(send_c.at[q], recv_c.at[q], out_c.at[q], in_c.at[q], EARLY_TILES)
            push(send_c.at[q], recv_c.at[q], out_c.at[q + 1], in_c.at[q + 1], LATE_TILES)

        return carry

    lax.fori_loop(0, PLANES, middle, 0)

    for load in loads[9:]:
        load.wait()
    row0 = row * KZL
    col0 = col * KXL - NX // 2

    def prepare(b, carry):
        n0 = pl.multiple_of(b * KXL, KXL)
        shape = (KXL, NY)
        ky = (lax.broadcasted_iota(jnp.int32, shape, 1) - NY // 2).astype(F32)
        kx = (lax.broadcasted_iota(jnp.int32, shape, 0) + col0).astype(F32)
        kz = (row0 + b).astype(F32)
        k1, squared, inv = waves_of(kx, ky, kz)
        lift = (2.0 * SHEAR_RATE * TIME_STEP) * ky * inv
        damp = (VISCOSITY * TIME_STEP) * squared
        for r in range(2):
            v0 = v_ref[0, r, pl.ds(n0, KXL), :]
            for m, k in enumerate((k1, ky, kz)):
                v = v_ref[m, r, pl.ds(n0, KXL), :]
                rate = k * lift * v0 - damp * v
                if m == 1:
                    rate = rate - (SHEAR_RATE * TIME_STEP) * v0
                rate = rate + REGISTER_WEIGHT * r_ref[m, r, pl.ds(n0, KXL), :]
                out_ref[m, r, pl.ds(n0, KXL), :] = v + UPDATE_WEIGHT * rate
        return carry

    lax.fori_loop(0, KZL, prepare, 0)
    moved = off_ref[...] * flag_ref[...]
    placing = placing_matrix(moved)
    block = lax.broadcasted_iota(jnp.int32, (1, COLS), 1)
    keep = jnp.sum(jnp.where(block == col, keep_ref[...], 0).astype(F32), axis=1, keepdims=True)
    stays = (moved == 0).astype(F32) * keep

    def tile_row(tile, r):
        return 2 * (tile % 2) + r // 4, 2 * (tile // 2) + r % 4 // 2, r % 2

    def gather(q, tiles):
        for tile in tiles:
            grid = grids.at[tile % 2]
            grid[...] = recv_c[q, :, tile].reshape(8 * DEVICES, 128).astype(F32)
            for r in range(8):
                e, j, s = tile_row(tile, r)
                points[q, e, s * 128:(s + 1) * 128, j * 128:(j + 1) * 128] = grid[
                    pl.ds(r, DEVICES, stride=8), :
                ].astype(BF16)


    def early(q, carry):
        drain(recv_c.at[q], in_c.at[q])
        gather(q, range(SENT))
        return carry

    lax.fori_loop(0, PLANES - 1, early, 0)
    for e in range(SENT):
        for h in range(2):
            cols = slice(h * 256, (h + 1) * 256)
            partial[h, e] = dot(yf_ref[:, :256], points[0, e, :, cols]) + dot(
                yf_ref[:, 256:512], points[1, e, :, cols]
            )
    scale = UPDATE_WEIGHT * TIME_STEP * FORWARD_SCALE

    def remesh_copy(w, place):
        shift = OFFSET_VALUES[place]
        return pltpu.make_async_remote_copy(
            src_ref=packs.at[w, place],
            dst_ref=arrived.at[w, place],
            send_sem=out_m.at[w, place],
            recv_sem=in_m.at[w, place],
            device_id=(row, col + shift),
            device_id_type=pl.DeviceIdType.MESH,
        )

    def inside(position):
        return (position >= 0) & (position < COLS)

    for w in range(4):
        h, u = w // 2, w % 2
        if u == 0:
            part = (EARLY_TILES, LATE_TILES)[h]
            drain(recv_c.at[PLANES - 1], in_c.at[PLANES - 1 + h], part)
            gather(PLANES - 1, range(part[0], part[0] + part[1]))
            for e in range(SENT):
                partial[h, e] += dot(yf_ref[:, 512:], points[2, e, :, h * 256:(h + 1) * 256])

        def project(b, carry):
            y0 = pl.multiple_of(b * 32, 32)
            shape = (32, 128)
            ky = (lax.broadcasted_iota(jnp.int32, shape, 0) + (y0 - NY // 2)).astype(F32)
            n = lax.broadcasted_iota(jnp.int32, shape, 1)
            kx = (n % KXL + col0).astype(F32)
            kz = (n // KXL + (row0 + w * 4)).astype(F32)
            k1, squared, inv = waves_of(kx, ky, kz)
            flat = kx * kx + kz * kz
            mean = flat == 0.0
            weight = scale / jnp.where(mean, 1.0, kx * kx + NORM * kz * kz)
            by_beta = (ky - (SHEAR_TIME / NORM) * kx) * inv * weight
            by_gamma = (ky * ky - flat * (1.0 / NORM)) * inv * weight
            c21 = ky * kx + SHEAR_TIME * kz * kz
            c22 = kz * kz + k1 * kx
            c23 = kz * (ky - SHEAR_TIME * k1)
            alone = jnp.where(mean, ky * scale, 0.0)
            for r in range(2):
                q1, q2, beta, gamma = [
                    partial[h, e, pl.ds((1 - r) * NY + y0, 32), u * 128:(u + 1) * 128] for e in range(SENT)
                ]
                p1 = (q1 + ky * q2) * weight
                p2 = by_beta * beta + by_gamma * gamma
                across = (q2 - SHEAR_TIME * q1) * (1.0 / NORM)
                n1 = c21 * p2 - kz * p1 + alone * (q1 + SHEAR_TIME * across)
                n2 = alone * (q2 - across) - c22 * p2 - SHEAR_TIME * kz * p1
                n3 = c23 * p2 + kx * p1 + alone * beta
                for m, part in enumerate((n1, n2, n3)):
                    rates[2 * m + r, pl.ds(y0, 32), :] = part if r == 0 else -part
            return carry

        lax.fori_loop(0, NY // 32, project, 0)
        rows = slice(w * 128, (w + 1) * 128)
        for m in range(3):
            for r in range(2):
                updated = out_ref[m, r, rows, :] + rates[2 * m + r].T
                out_ref[m, r, rows, :] = updated * stays
                packed = dot(updated.astype(BF16), placing, NT)
                parts = [packed[k * 32:(k + 1) * 32] for k in range(4)]
                for k, part in enumerate(lane_blocks(parts)):
                    packs[w, k, 2 * m + r] = part.astype(BF16)
        for place, shift in enumerate(OFFSET_VALUES):

            @pl.when(inside(col + shift))
            def _():
                remesh_copy(w, place).start()

            @pl.when(jnp.logical_not(inside(col - shift)))
            def _():
                arrived[w, place] = jnp.zeros((6, 32, 128), BF16)

    for q in range(PLANES):
        drain(send_b.at[q], out_b.at[q])
        if q < PLANES - 1:
            drain(send_c.at[q], out_c.at[q])
    for h, part in enumerate((EARLY_TILES, LATE_TILES)):
        drain(send_c.at[PLANES - 1], out_c.at[PLANES - 1 + h], part)
    kept = (placing.astype(F32) * keep).astype(BF16)
    for w in range(4):
        for place, shift in enumerate(OFFSET_VALUES):

            @pl.when(inside(col - shift))
            def _():
                remesh_copy(w, place).wait_recv()

        for m in range(3):
            for r in range(2):
                parts = lane_blocks([arrived[w, place, 2 * m + r].astype(F32) for place in range(4)])
                part = jnp.concatenate(parts, axis=0).astype(BF16)
                rows = slice(w * 128, (w + 1) * 128)
                out_ref[m, r, rows, :] += dot(part, kept)

    for w in range(4):
        for place, shift in enumerate(OFFSET_VALUES):

            @pl.when(inside(col + shift))
            def _():
                remesh_copy(w, place).wait_send()


def local(velocity, register, offsets, remesh_flag, keep_blocks):
    constants = tables()
    velocity = velocity.reshape(3, 2, MODES, NY)
    register = register.reshape(3, 2, MODES, NY)
    anywhere = pl.BlockSpec(memory_space=pltpu.HBM)
    vmem = pl.BlockSpec(memory_space=pltpu.VMEM)
    out = pl.pallas_call(
        step_kernel,
        in_specs=[anywhere] * 11,
        out_specs=vmem,
        out_shape=pltpu.VMEM((3, 2, MODES, NY), F32),
        scratch_shapes=[
            pltpu.VMEM(velocity.shape, F32),
            pltpu.VMEM(register.shape, F32),
            *[pltpu.VMEM(t.shape, BF16) for t in constants],
            pltpu.VMEM((1, NY), jnp.int32),
            pltpu.VMEM((1, NY), jnp.int32),
            pltpu.VMEM((1, COLS), jnp.int32),
            pltpu.VMEM((3, MODES, 2 * NY), BF16),
            pltpu.VMEM((2, 8 * DEVICES, 128), F32),
            pltpu.VMEM((PLANES, DEVICES, 3, 8, 128), BF16),
            pltpu.VMEM((PLANES, DEVICES, 3, 8, 128), BF16),
            pltpu.VMEM((3, 256, NX), BF16),
            pltpu.VMEM((3, 512, MX), BF16),
            pltpu.VMEM((PRODUCTS, 256, 2 * MX), BF16),
            pltpu.VMEM((PLANES, DEVICES, SENT, 8, 128), BF16),
            pltpu.VMEM((PLANES, DEVICES, SENT, 8, 128), BF16),
            pltpu.VMEM((PLANES, SENT, 2 * DEVICES, MODES), BF16),
            pltpu.VMEM((2, SENT, 2 * NY, 256), F32),
            pltpu.VMEM((PRODUCTS, 256, NX), F32),
            pltpu.VMEM((6, NY, 128), F32),
            pltpu.VMEM((4, 4, 6, 32, 128), BF16),
            pltpu.VMEM((4, 4, 6, 32, 128), BF16),
            pltpu.SemaphoreType.DMA((14,)),
            pltpu.SemaphoreType.DMA((PLANES,)),
            pltpu.SemaphoreType.DMA((PLANES,)),
            pltpu.SemaphoreType.DMA((PLANES + 1,)),
            pltpu.SemaphoreType.DMA((PLANES + 1,)),
            pltpu.SemaphoreType.DMA((4, 4)),
            pltpu.SemaphoreType.DMA((4, 4)),
        ],
        compiler_params=pltpu.CompilerParams(
            vmem_limit_bytes=VMEM_LIMIT, collective_id=0, has_side_effects=True
        ),
        name="step",
    )(
        velocity,
        register,
        *constants,
        offsets.reshape(1, NY),
        remesh_flag.reshape(1, NY),
        keep_blocks.reshape(1, COLS),
    )
    return out.reshape(3, 2, KZL, KXL, NY)


def solution(mesh):
    placed = (P(None, None, "row", "col", None), P(None, None, "row", "col", None), P(), P(), P())
    return jax.shard_map(
        local,
        mesh=mesh,
        in_specs=placed,
        out_specs=P(None, None, "row", "col", None),
        check_vma=False,
    )
```
